1024 devices in a mesh: space: 16 (over x, y), sub: 64 (over z, core).
Axes of the slice: x: 4, y: 4, z: 32, core: 2. Of those that a mesh axis runs over, the one named last changes fastest.
Arguments:
- positions: float32 [3, 16, 4096, 128], P(None, 'space', 'sub'), may hold values from 0 to 1.5
- masses: float32 [16, 4096, 128], P('space', 'sub'), may hold values from 0.1 to 1
- occupancy: int32 [16, 4096], P('space', 'sub'), may hold values from 1 to 128
- export_slots: int32 [16, 2048], P('space', 'sub'), may hold values from 0 to 63, as said below
- export_count: int32 [16, 64], P('space', 'sub'), may hold values from 16 to 32
- pair_list: int32 [2, 16, 4096], P(None, 'space', 'sub'), may hold values from 0 to 319, as said below
- pair_count: int32 [16, 64], P('space', 'sub'), may hold values from 16 to 64
Outputs:
- forces: float32 [3, 16, 4096, 128], P(None, 'space', 'sub')
The draws below stay inside these ranges and needn't reach their ends.
Inputs may be any that keep to these rules, and one draw needn't show every extreme that they name: `export_slots`: the 32 entries of one device are distinct own-leaf indices. `pair_list`: row 0 is a target own leaf, below 64; row 1 is a source pool leaf, below 320, never equal to the target.
All inputs are finite; a program needn't handle non-finite values.
Results may differ from the reference program's by a relative error of at most 0.0003.
Values sent between devices are 32-bit elements; how exact they have to be, the bound alone decides.
A program may use at most 32 MiB of HBM per device.

```python
import math
import jax
import jax.numpy as jnp
from jax import lax

LEAF = 128
LEAVES = 64
G = 32
PAIRS = 64
N_SPACE = 16
N_SUB = 64


def draw_export_slots(key, part):
    keys = jax.random.split(jax.random.fold_in(key, 7), N_SPACE * N_SUB)
    chosen = jax.vmap(lambda single: jax.random.permutation(single, LEAVES)[:G])(keys)
    return chosen.reshape(N_SPACE, N_SUB * G).astype(jnp.int32)


def draw_pair_list(key, part):
    first, second = jax.random.split(jax.random.fold_in(key, 11))
    targets = jax.random.randint(first, (N_SPACE, N_SUB * PAIRS), 0, LEAVES, dtype=jnp.int32)
    drawn = jax.random.randint(second, (N_SPACE, N_SUB * PAIRS), 0, LEAVES + 8 * G - 1, dtype=jnp.int32)
    sources = drawn + (drawn >= targets).astype(jnp.int32)
    return jnp.stack([targets, sources]).astype(jnp.int32)


def plant(values, stream_key, smallest, largest):
    spot = [jax.random.randint(jax.random.fold_in(stream_key, axis), (), 0, length) for axis, length in enumerate(values.shape)]
    longest = values.shape.index(max(values.shape))
    neighbour = spot[:longest] + [(spot[longest] + 1) % values.shape[longest]] + spot[longest + 1:]
    return values.at[tuple(spot)].set(smallest).at[tuple(neighbour)].set(largest)


def block_levels(stream_key, extent, cuts, least, high):
    level, own = 1.0, jax.random.fold_in(stream_key, 6)
    for position, shards_of in cuts:
        draws = jnp.exp(jax.random.uniform(jax.random.fold_in(own, position), (shards_of,), jnp.float32, least / len(cuts), high / len(cuts)))
        level = level * jnp.repeat(draws, extent[position] // shards_of).reshape([-1 if axis == position else 1 for axis in range(len(extent))])
    return level


def setup_inputs(seed: int = 0) -> dict:
    splits = jax.random.split(jax.random.key(seed), 8)
    positions = jnp.clip(1.5 * jax.random.uniform(splits[0], (3, N_SPACE, N_SUB * LEAVES, LEAF), jnp.float32) ** block_levels(splits[0], (3, N_SPACE, N_SUB * LEAVES, LEAF), ((1, 16), (2, 64)), -0.2, 0.2), 0.0, 1.5)
    masses = jnp.clip(jnp.exp(math.log(1.0) - 2.3025851 * jax.random.uniform(splits[1], (N_SPACE, N_SUB * LEAVES, LEAF), jnp.float32) ** block_levels(splits[1], (N_SPACE, N_SUB * LEAVES, LEAF), ((0, 16), (1, 64)), -0.2, 0.2)), 0.1, 1.0)
    occupancy = plant(jax.random.randint(splits[2], (N_SPACE, N_SUB * LEAVES), 1, LEAF + 1), jax.random.fold_in(splits[2], 1), 1, LEAF).astype(jnp.int32)
    export_slots = draw_export_slots(jax.random.fold_in(splits[7], 71), 0)
    export_count = plant(jax.random.randint(splits[4], (N_SPACE, N_SUB), G // 2, G + 1), jax.random.fold_in(splits[4], 1), G // 2, G).astype(jnp.int32)
    pair_list = draw_pair_list(jax.random.fold_in(splits[7], 71), 0)
    pair_count = plant(jax.random.randint(splits[6], (N_SPACE, N_SUB), PAIRS // 4, PAIRS + 1), jax.random.fold_in(splits[6], 1), PAIRS // 4, PAIRS).astype(jnp.int32)
    return dict(positions=positions, masses=masses, occupancy=occupancy, export_slots=export_slots, export_count=export_count, pair_list=pair_list, pair_count=pair_count)


OFFSETS = ((-1, -1), (-1, 0), (-1, 1), (0, -1), (0, 1), (1, -1), (1, 0), (1, 1))
SOFTEN = 0.05
PRECISE = lax.Precision.HIGHEST

def pair_block(target_pos, target_mass, source_pos, source_mass):
    separation = source_pos[:, :, None, :] - target_pos[:, :, :, None]
    distance = lax.optimization_barrier(jnp.sum(separation * separation, axis=0))
    falloff = jnp.maximum(1.0 - distance, 0.0)
    softened = distance + SOFTEN
    weight = target_mass[:, :, None] * source_mass[:, None, :] * falloff * falloff / (softened * jnp.sqrt(softened))
    row_total = lax.optimization_barrier(jnp.sum(weight, axis=2))
    col_total = lax.optimization_barrier(jnp.sum(weight, axis=1))
    on_target = jnp.einsum('bij,cbj->cbi', weight, source_pos, precision=PRECISE) - target_pos * row_total[None]
    on_source = jnp.einsum('bij,cbi->cbj', weight, target_pos, precision=PRECISE) - source_pos * col_total[None]
    return (on_target, on_source)

def device_forces(pool_pos, pool_mass, pair_rows, pair_total):
    own_index = jnp.arange(LEAVES, dtype=jnp.int32)
    live = (jnp.arange(PAIRS, dtype=jnp.int32) < pair_total).astype(jnp.float32)
    targets = jnp.concatenate([own_index, pair_rows[0]])
    sources = jnp.concatenate([own_index, pair_rows[1]])
    target_scale = jnp.concatenate([jnp.ones((LEAVES,), jnp.float32), live])
    source_scale = jnp.concatenate([jnp.zeros((LEAVES,), jnp.float32), live])

    def one_block(indices):
        tgt_rows, src_rows = indices
        return pair_block(pool_pos[:, tgt_rows], pool_mass[tgt_rows], pool_pos[:, src_rows], pool_mass[src_rows])
    on_target, on_source = lax.map(one_block, (targets.reshape(8, -1), sources.reshape(8, -1)))
    on_target = jnp.moveaxis(on_target, 0, 1).reshape(3, -1, LEAF)
    on_source = jnp.moveaxis(on_source, 0, 1).reshape(3, -1, LEAF)
    pool_force = jnp.zeros((3, pool_mass.shape[0], LEAF), jnp.float32)
    pool_force = pool_force.at[:, targets].add(on_target * target_scale[None, :, None])
    pool_force = pool_force.at[:, sources].add(on_source * source_scale[None, :, None])
    return pool_force

def reference(positions, masses, occupancy, export_slots, export_count, pair_list, pair_count):
    slot_index = lax.broadcasted_iota(jnp.int32, masses.shape, 2)
    live_mass = jnp.where(slot_index < occupancy[:, :, None], masses, 0.0)
    grid_pos = positions.reshape(3, N_SPACE, N_SUB, LEAVES, LEAF)
    grid_mass = live_mass.reshape(N_SPACE, N_SUB, LEAVES, LEAF)
    slots = export_slots.reshape(N_SPACE, N_SUB, G)
    keep = (jnp.arange(G, dtype=jnp.int32)[None, None, :] < export_count[:, :, None]).astype(jnp.float32)
    pos_index = jnp.broadcast_to(slots[None, :, :, :, None], (3, N_SPACE, N_SUB, G, LEAF))
    mass_index = jnp.broadcast_to(slots[:, :, :, None], (N_SPACE, N_SUB, G, LEAF))
    sent_pos = jnp.take_along_axis(grid_pos, pos_index, axis=3)
    sent_mass = jnp.take_along_axis(grid_mass, mass_index, axis=2) * keep[:, :, :, None]
    pos_list = [grid_pos]
    mass_list = [grid_mass]
    for space_step, sub_step in OFFSETS:
        pos_list.append(jnp.roll(sent_pos, (-space_step, -sub_step), axis=(1, 2)))
        mass_list.append(jnp.roll(sent_mass, (-space_step, -sub_step), axis=(0, 1)))
    pool_pos = jnp.concatenate(pos_list, axis=3)
    pool_mass = jnp.concatenate(mass_list, axis=2)
    pool_size = LEAVES + 8 * G
    device_total = N_SPACE * N_SUB
    dev_pos = jnp.moveaxis(pool_pos.reshape(3, device_total, pool_size, LEAF), 1, 0)
    dev_mass = pool_mass.reshape(device_total, pool_size, LEAF)
    dev_pairs = jnp.moveaxis(pair_list.reshape(2, device_total, PAIRS), 1, 0)
    dev_count = pair_count.reshape(device_total)

    def per_device(items):
        return device_forces(items[0], items[1], items[2], items[3])
    pool_force = lax.map(per_device, (dev_pos, dev_mass, dev_pairs, dev_count))
    pool_force = pool_force.reshape(N_SPACE, N_SUB, 3, pool_size, LEAF)
    own_force = pool_force[:, :, :, :LEAVES]
    returned = jnp.zeros((N_SPACE, N_SUB, 3, G, LEAF), jnp.float32)
    for order, (space_step, sub_step) in enumerate(OFFSETS):
        block = pool_force[:, :, :, LEAVES + order * G:LEAVES + (order + 1) * G]
        returned = returned + jnp.roll(block, (space_step, sub_step), axis=(0, 1))
    picker = (slots[:, :, :, None] == jnp.arange(LEAVES, dtype=jnp.int32)[None, None, None, :]).astype(jnp.float32)
    own_force = own_force + jnp.einsum('sbgl,sbcgp->sbclp', picker, returned, precision=PRECISE)
    forces = jnp.moveaxis(own_force, 2, 0)
    return forces.reshape(3, N_SPACE, N_SUB * LEAVES, LEAF)
```

```python
import functools

import jax
import jax.numpy as jnp
from jax import lax
from jax.experimental import pallas as pl
from jax.experimental.pallas import tpu as pltpu
from jax.sharding import PartitionSpec as P

OFFSETS = ((-1, -1), (-1, 0), (-1, 1), (0, -1), (0, 1), (1, -1), (1, 0), (1, 1))
SOFTEN = 0.05
CENTRE = 0.75
MESH = pl.DeviceIdType.MESH
F32 = jnp.float32
BF16 = jnp.bfloat16
UNROLL = 4


def split3(x):
    h = x.astype(BF16).astype(F32)
    rest = x - h
    m = rest.astype(BF16).astype(F32)
    return h, m, rest - m


def pieces(leaf):
    twice = jnp.concatenate([leaf, leaf], axis=0)
    row = lax.broadcasted_iota(jnp.int32, (8, 128), 0)
    low = row < 4
    last = (row == 3) | (row == 7)
    centred = jnp.where(last, 0.0, twice - CENTRE)
    return twice, centred, low, last, leaf[3:4, :]


def squared(centred, last):
    q = 0.5 * jnp.sum(centred * centred, axis=0, keepdims=True)
    return split3(jnp.where(last, q, centred))


def target_features(centred, low, last):
    h, m, l = squared(centred, last)
    h1 = jnp.where(last, 1.0, h)
    m1 = jnp.where(last, 1.0, m)
    rows = [jnp.where(low, h, m), jnp.where(low, l, h1), jnp.where(low, h1, m1), jnp.zeros_like(h)]
    return jnp.concatenate(rows, axis=0)


def source_features(centred, low, last):
    h, m, l = squared(centred, last)
    head = jnp.where(last, 1.0, -2.0 * h)
    rows = [
        head,
        jnp.where(low, head, jnp.where(last, h, -2.0 * m)),
        jnp.where(low, jnp.where(last, m, -2.0 * l), jnp.where(last, l, -2.0 * m)),
        jnp.zeros_like(h),
    ]
    return jnp.concatenate(rows, axis=0)


def moments(centred, low, last, mass):
    h, m, l = split3(jnp.where(last, 1.0, centred) * mass)
    return jnp.concatenate([jnp.where(low, h, m), jnp.where(low, l, 0.0)], axis=0).astype(BF16)


def weights(distance):
    falloff = jnp.maximum(1.0 - distance, 0.0)
    root = lax.rsqrt(distance + SOFTEN)
    scaled = falloff * root
    return scaled * scaled * root


def halves(w):
    hi = w.astype(BF16)
    return hi, (w - hi.astype(F32)).astype(BF16)


def force(total, centred, mass):
    both = total[0:8] + total[8:16]
    both = both + pltpu.roll(both, 4, 0)
    return mass * (both - centred * both[3:4, :])


def dot(a, b):
    return jnp.dot(a, b, preferred_element_type=F32)


def dot_t(a, b):
    return lax.dot_general(a, b, (((1,), (1,)), ((), ())), preferred_element_type=F32)


def pipeline(groups, first, second, bufs):
    first(0, bufs[0])

    def step(i, carry):
        first(2 * i + 1, bufs[1])
        second(2 * i, bufs[0])
        first(2 * i + 2, bufs[0])
        second(2 * i + 1, bufs[1])
        return carry

    lax.fori_loop(0, groups // 2 - 1, step, 0)
    first(groups - 1, bufs[1])
    second(groups - 2, bufs[0])
    second(groups - 1, bufs[1])


def kernel(
    shape,
    pos_hbm, mass_hbm, occ_hbm, slots_hbm, ecount_hbm, pairs_hbm, pcount_hbm,
    out_ref,
    pos_v, mass_v, occ_s, slots_s, ecount_s, pairs_s, pcount_s, slots_v, pairs_v,
    sent, pool, target_t, hi0, lo0, hi1, lo1, self_f, pair_f, ghost_f, returned, acc,
    in_sem, send_sem, recv_sem, send2_sem, recv2_sem,
):
    n_space, n_sub = shape
    leaves = pos_v.shape[1]
    g_total = sent.shape[0]
    pair_slots = pairs_v.shape[2]
    s = lax.axis_index("space")
    r = lax.axis_index("sub")

    def place(a, b):
        return (lax.rem(s + a + n_space, n_space), lax.rem(r + b + n_sub, n_sub))

    loads = [
        pltpu.make_async_copy(src, dst, in_sem.at[i])
        for i, (src, dst) in enumerate(
            [
                (pos_hbm.at[:, 0], pos_v),
                (mass_hbm.at[0], mass_v),
                (slots_hbm, slots_s),
                (occ_hbm, occ_s),
                (ecount_hbm, ecount_s),
                (pairs_hbm, pairs_s),
                (pcount_hbm, pcount_s),
                (slots_hbm, slots_v),
                (pairs_hbm, pairs_v),
            ]
        )
    ]
    for load in loads:
        load.start()
    barrier = pltpu.get_barrier_semaphore()
    for a, b in OFFSETS:
        pl.semaphore_signal(barrier, inc=1, device_id=place(a, b), device_id_type=MESH)
    for load in loads:
        load.wait()

    lane = lax.broadcasted_iota(jnp.int32, (1, 128), 1)
    exported = ecount_s[0, 0]

    def gather(i, carry):
        for j in range(4):
            g = i * 4 + j
            slot = slots_s[0, g]
            for c in range(3):
                sent[g, pl.ds(c, 1), :] = pos_v[c, pl.ds(slot, 1), :]
            live = jnp.where(g < exported, occ_s[0, slot], 0)
            sent[g, pl.ds(3, 1), :] = jnp.where(lane < live, mass_v[pl.ds(slot, 1), :], 0.0)
        return carry

    lax.fori_loop(0, g_total // 4, gather, 0)
    pl.semaphore_wait(barrier, len(OFFSETS))

    out_copies = []
    for k, (a, b) in enumerate(OFFSETS):
        copy = pltpu.make_async_remote_copy(
            src_ref=sent,
            dst_ref=pool.at[pl.ds(leaves + k * g_total, g_total)],
            send_sem=send_sem.at[k],
            recv_sem=recv_sem.at[k],
            device_id=place(-a, -b),
            device_id_type=MESH,
        )
        copy.start()
        out_copies.append(copy)

    def own(i, carry):
        for j in range(4):
            leaf = i * 4 + j
            for c in range(3):
                pool[leaf, pl.ds(c, 1), :] = pos_v[c, pl.ds(leaf, 1), :]
            pool[leaf, pl.ds(3, 1), :] = jnp.where(
                lane < occ_s[0, leaf], mass_v[pl.ds(leaf, 1), :], 0.0
            )
        return carry

    lax.fori_loop(0, leaves // 4, own, 0)

    def self_first(group, buf):
        hi, lo = buf
        for j in range(UNROLL):
            leaf = group * UNROLL + j
            _, centred, low, last, _ = pieces(pool[leaf])
            at = target_features(centred, low, last).T.astype(BF16)
            target_t[leaf] = at
            hi[j], lo[j] = halves(weights(dot(at, source_features(centred, low, last).astype(BF16))))

    def self_second(group, buf):
        hi, lo = buf
        for j in range(UNROLL):
            leaf = group * UNROLL + j
            _, centred, low, last, mass = pieces(pool[leaf])
            mom = moments(centred, low, last, mass)
            f = force(dot(mom, hi[j]) + dot(mom, lo[j]), centred, mass)
            for c in range(3):
                self_f[c, pl.ds(leaf, 1), :] = f[c : c + 1, :]

    bufs = ((hi0, lo0), (hi1, lo1))
    pipeline(leaves // UNROLL, self_first, self_second, bufs)

    for copy in out_copies:
        copy.wait_recv()

    def pair_first(group, buf):
        hi, lo = buf
        for j in range(UNROLL):
            p = group * UNROLL + j
            _, centred, low, last, _ = pieces(pool[pairs_s[1, 0, p]])
            src = source_features(centred, low, last).astype(BF16)
            hi[j], lo[j] = halves(weights(dot(target_t[pairs_s[0, 0, p]], src)))

    def pair_second(group, buf):
        hi, lo = buf
        for j in range(UNROLL):
            p = group * UNROLL + j
            _, t_centred, low, last, t_mass = pieces(pool[pairs_s[0, 0, p]])
            _, s_centred, low, last, s_mass = pieces(pool[pairs_s[1, 0, p]])
            t_mom = moments(t_centred, low, last, t_mass)
            s_mom = moments(s_centred, low, last, s_mass)
            on_target = force(dot_t(s_mom, hi[j]) + dot_t(s_mom, lo[j]), t_centred, t_mass)
            on_source = force(dot(t_mom, hi[j]) + dot(t_mom, lo[j]), s_centred, s_mass)
            for c in range(3):
                pair_f[c, pl.ds(p, 1), :] = on_target[c : c + 1, :]
                pair_f[c, pl.ds(pair_slots + p, 1), :] = on_source[c : c + 1, :]

    pipeline(pair_slots // UNROLL, pair_first, pair_second, bufs)

    key = jnp.concatenate([pairs_v[0], pairs_v[1]], axis=1)
    slot = lax.broadcasted_iota(jnp.int32, (1, 2 * pair_slots), 1)
    slot = jnp.where(slot < pair_slots, slot, slot - pair_slots)
    key = jnp.where(slot < pcount_s[0, 0], key, -1)
    split = [piece.astype(BF16) for piece in split3(jnp.concatenate([pair_f[0], pair_f[1], pair_f[2]], axis=1))]

    def scatter(start, rows):
        index = lax.broadcasted_iota(jnp.int32, (rows, 2 * pair_slots), 0) + start
        pick = jnp.where(index == key, 1.0, 0.0).astype(BF16)
        return dot(pick, split[0]) + dot(pick, split[1]) + dot(pick, split[2])

    ghosts = scatter(leaves, 8 * g_total)
    for k in range(8):
        for c in range(3):
            ghost_f[k, c] = ghosts[k * g_total : (k + 1) * g_total, c * 128 : (c + 1) * 128]
    back_copies = []
    for k, (a, b) in enumerate(OFFSETS):
        copy = pltpu.make_async_remote_copy(
            src_ref=ghost_f.at[k],
            dst_ref=returned.at[k],
            send_sem=send2_sem.at[k],
            recv_sem=recv2_sem.at[k],
            device_id=place(a, b),
            device_id_type=MESH,
        )
        copy.start()
        back_copies.append(copy)

    mine = scatter(0, leaves)
    for c in range(3):
        acc[c] = mine[:, c * 128 : (c + 1) * 128] + self_f[c]
    for copy in out_copies:
        copy.wait_send()
    pick = jnp.where(
        lax.broadcasted_iota(jnp.int32, (leaves, g_total), 0) == slots_v[...], 1.0, 0.0
    ).astype(BF16)
    for copy in back_copies:
        copy.wait_recv()
    for c in range(3):
        total = returned[0, c]
        for k in range(1, 8):
            total = total + returned[k, c]
        h, m, l = split3(total)
        out_ref[c, 0] = (
            acc[c]
            + dot(pick, h.astype(BF16))
            + dot(pick, m.astype(BF16))
            + dot(pick, l.astype(BF16))
        )
    for copy in back_copies:
        copy.wait_send()


def local(shape, positions, masses, occupancy, export_slots, export_count, pair_list, pair_count):
    leaves, width = masses.shape[1:]
    g_total = export_slots.shape[1]
    pair_slots = pair_list.shape[2]
    anywhere = pl.BlockSpec(memory_space=pl.ANY)
    return pl.pallas_call(
        functools.partial(kernel, shape),
        out_shape=jax.ShapeDtypeStruct(positions.shape, F32),
        in_specs=[anywhere] * 7,
        out_specs=pl.BlockSpec(memory_space=pltpu.VMEM),
        scratch_shapes=[
            pltpu.VMEM((3, leaves, width), F32),
            pltpu.VMEM((leaves, width), F32),
            pltpu.SMEM((1, leaves), jnp.int32),
            pltpu.SMEM((1, g_total), jnp.int32),
            pltpu.SMEM((1, 1), jnp.int32),
            pltpu.SMEM((2, 1, pair_slots), jnp.int32),
            pltpu.SMEM((1, 1), jnp.int32),
            pltpu.VMEM((1, g_total), jnp.int32),
            pltpu.VMEM((2, 1, pair_slots), jnp.int32),
            pltpu.VMEM((g_total, 4, width), F32),
            pltpu.VMEM((leaves + 8 * g_total, 4, width), F32),
            pltpu.VMEM((leaves, width, 32), BF16),
            pltpu.VMEM((UNROLL, width, width), BF16),
            pltpu.VMEM((UNROLL, width, width), BF16),
            pltpu.VMEM((UNROLL, width, width), BF16),
            pltpu.VMEM((UNROLL, width, width), BF16),
            pltpu.VMEM((3, leaves, width), F32),
            pltpu.VMEM((3, 2 * pair_slots, width), F32),
            pltpu.VMEM((8, 3, g_total, width), F32),
            pltpu.VMEM((8, 3, g_total, width), F32),
            pltpu.VMEM((3, leaves, width), F32),
            pltpu.SemaphoreType.DMA((9,)),
            pltpu.SemaphoreType.DMA((8,)),
            pltpu.SemaphoreType.DMA((8,)),
            pltpu.SemaphoreType.DMA((8,)),
            pltpu.SemaphoreType.DMA((8,)),
        ],
        compiler_params=pltpu.CompilerParams(collective_id=0, has_side_effects=True),
    )(positions, masses, occupancy, export_slots, export_count, pair_list, pair_count)


def solution(mesh):
    return jax.shard_map(
        functools.partial(local, (mesh.shape["space"], mesh.shape["sub"])),
        mesh=mesh,
        in_specs=(
            P(None, "space", "sub", None),
            P("space", "sub", None),
            P("space", "sub"),
            P("space", "sub"),
            P("space", "sub"),
            P(None, "space", "sub"),
            P("space", "sub"),
        ),
        out_specs=P(None, "space", "sub", None),
        check_vma=False,
    )
```

```python
import functools

import jax
import jax.numpy as jnp
from jax import lax
from jax.experimental import pallas as pl
from jax.experimental.pallas import tpu as pltpu
from jax.sharding import PartitionSpec as P

OFFSETS = ((-1, -1), (-1, 0), (-1, 1), (0, -1), (0, 1), (1, -1), (1, 0), (1, 1))
SOFTEN = 0.05
CENTRE = 0.75
MESH = pl.DeviceIdType.MESH
F32 = jnp.float32
BF16 = jnp.bfloat16
UNROLL = 4


def split3(x):
    h = x.astype(BF16).astype(F32)
    rest = x - h
    m = rest.astype(BF16).astype(F32)
    return h, m, rest - m


def rows_of():
    row = lax.broadcasted_iota(jnp.int32, (8, 128), 0)
    return row < 4, (row == 3) | (row == 7)


def centre(leaf, last):
    return jnp.where(last, 0.0, jnp.concatenate([leaf, leaf], axis=0) - CENTRE)


def squared(centred, last, extra):
    q = 0.5 * jnp.sum(centred * centred, axis=0, keepdims=True) + extra
    return split3(jnp.where(last, q, centred))


def target_features(centred, low, last):
    h, m, l = squared(centred, last, 0.0)
    h1 = jnp.where(last, 1.0, h)
    m1 = jnp.where(last, 1.0, m)
    rows = [jnp.where(low, h, m), jnp.where(low, l, h1), jnp.where(low, h1, m1), jnp.zeros_like(h)]
    return jnp.concatenate(rows, axis=0).astype(BF16)


def source_features(centred, low, last):
    h, m, l = squared(centred, last, SOFTEN)
    head = jnp.where(last, 1.0, -2.0 * h)
    rows = [
        head,
        jnp.where(low, head, jnp.where(last, h, -2.0 * m)),
        jnp.where(low, jnp.where(last, m, -2.0 * l), jnp.where(last, l, -2.0 * m)),
        jnp.zeros_like(h),
    ]
    return jnp.concatenate(rows, axis=0).astype(BF16)


def moments(centred, low, last, mass):
    h, m, l = split3(jnp.where(last, 1.0, centred) * mass)
    return jnp.concatenate([jnp.where(low, h, m), jnp.where(low, l, 0.0)], axis=0).astype(BF16)


def weights(softened):
    falloff = jnp.maximum((1.0 + SOFTEN) - softened, 0.0)
    root = lax.rsqrt(softened)
    scaled = falloff * root
    return scaled * scaled * root


def force(total, centred, mass):
    both = total[0:8] + total[8:16]
    both = both + pltpu.roll(both, 4, 0)
    return mass * (both - centred * both[3:4, :])


def dot(a, b):
    return jnp.dot(a, b, preferred_element_type=F32)


def dot_t(a, b):
    return lax.dot_general(a, b, (((1,), (1,)), ((), ())), preferred_element_type=F32)


def both_weights(left, right, source_left, source_right, buf, j):
    lane = lax.broadcasted_iota(jnp.int32, left.shape, 1)
    target = jnp.where(lane < 32, left, right)
    zero = jnp.zeros_like(source_left)
    source = jnp.concatenate(
        [
            jnp.concatenate([source_left, zero], axis=1),
            jnp.concatenate([zero, source_right], axis=1),
        ],
        axis=0,
    )
    w = weights(dot(target, source))
    hi = w.astype(BF16)
    lo = (w - hi.astype(F32)).astype(BF16)
    for i in range(2):
        buf[j + i, :, 0:128] = hi[:, i * 128 : (i + 1) * 128]
        buf[j + i, :, 128:256] = lo[:, i * 128 : (i + 1) * 128]


def folded(total):
    return total[:, 0:128] + total[:, 128:256]


def pipeline(groups, first, second, bufs):
    first(0, bufs[0])

    def step(i, carry):
        first(2 * i + 1, bufs[1])
        second(2 * i, bufs[0])
        first(2 * i + 2, bufs[0])
        second(2 * i + 1, bufs[1])
        return carry

    lax.fori_loop(0, groups // 2 - 1, step, 0)
    first(groups - 1, bufs[1])
    second(groups - 2, bufs[0])
    second(groups - 1, bufs[1])


def slot_of(a, b):
    if a == 0:
        return 3 + (b + 1) // 2
    return b + 1 if a < 0 else b + 6


def kernel(
    shape,
    pos_hbm, mass_hbm, occ_hbm, slots_hbm, ecount_hbm, pairs_hbm, pcount_hbm,
    out_ref,
    pos_v, mass_v, occ_s, slots_s, ecount_s, pairs_s, pcount_s, slots_v, pairs_v,
    sent, pool, target_t, moment_o, buf0, buf1, self_f, pair_f, ghost_f, via, passed, returned, acc,
    in_sem, send_sem, recv_sem, send2_sem, recv2_sem,
):
    n_space, n_sub = shape
    leaves = pos_v.shape[1]
    g_total = sent.shape[0]
    pair_slots = pairs_v.shape[2]
    s = lax.axis_index("space")
    r = lax.axis_index("sub")
    inner = 1 - 2 * lax.rem(r, 2)
    outer = -inner

    def place(a, b):
        return (lax.rem(s + a + n_space, n_space), lax.rem(r + b + n_sub, n_sub))

    loads = [
        pltpu.make_async_copy(src, dst, in_sem.at[i])
        for i, (src, dst) in enumerate(
            [
                (slots_hbm, slots_s),
                (occ_hbm, occ_s),
                (ecount_hbm, ecount_s),
                (pos_hbm.at[:, 0], pos_v),
                (mass_hbm.at[0], mass_v),
                (pairs_hbm, pairs_s),
                (pcount_hbm, pcount_s),
                (slots_hbm, slots_v),
                (pairs_hbm, pairs_v),
            ]
        )
    ]
    for load in loads:
        load.start()
    barrier = pltpu.get_barrier_semaphore()
    for a, b in OFFSETS:
        pl.semaphore_signal(barrier, inc=1, device_id=place(a, b), device_id_type=MESH)
    for load in loads:
        load.wait()

    lane = lax.broadcasted_iota(jnp.int32, (1, 128), 1)
    exported = ecount_s[0, 0]

    def gather(i, carry):
        for j in range(8):
            g = i * 8 + j
            slot = slots_s[0, g]
            for c in range(3):
                sent[g, pl.ds(c, 1), :] = pos_v[c, pl.ds(slot, 1), :]
            live = jnp.where(g < exported, occ_s[0, slot], 0)
            sent[g, pl.ds(3, 1), :] = jnp.where(lane < live, mass_v[pl.ds(slot, 1), :], 0.0)
        return carry

    lax.fori_loop(0, g_total // 8, gather, 0)
    pl.semaphore_wait(barrier, len(OFFSETS))

    def remote(src, dst, send, recv, role, a, b):
        copy = pltpu.make_async_remote_copy(
            src_ref=src,
            dst_ref=dst,
            send_sem=send.at[role],
            recv_sem=recv.at[role],
            device_id=place(a, b),
            device_id_type=MESH,
        )
        copy.start()
        return copy

    def ghosts_at(slot):
        return pool.at[pl.ds(leaves + slot * g_total, g_total)]

    def export(role, a, b, slot, src=sent):
        return remote(src, ghosts_at(slot), send_sem, recv_sem, role, a, b)

    ahead = [export(0, 1, 0, slot_of(-1, 0)), export(1, -1, 0, slot_of(1, 0))]
    out_copies = [
        export(4, 1, outer, inner + 1),
        export(5, -1, outer, inner + 6),
        export(3, 0, outer, 3 + (inner + 1) // 2),
        export(2, 0, inner, 3 + (outer + 1) // 2),
    ]

    def own(i, carry):
        for j in range(8):
            leaf = i * 8 + j
            for c in range(3):
                pool[leaf, pl.ds(c, 1), :] = pos_v[c, pl.ds(leaf, 1), :]
            pool[leaf, pl.ds(3, 1), :] = jnp.where(
                lane < occ_s[0, leaf], mass_v[pl.ds(leaf, 1), :], 0.0
            )
        return carry

    lax.fori_loop(0, leaves // 8, own, 0)

    def self_first(group, buf):
        low, last = rows_of()
        for j in range(0, UNROLL, 2):
            targets, sources = [], []
            for leaf in (group * UNROLL + j, group * UNROLL + j + 1):
                centred = centre(pool[leaf], last)
                feature = target_features(centred, low, last)
                target = jnp.concatenate([feature, feature], axis=0).T
                target_t[leaf] = target
                targets.append(target)
                sources.append(source_features(centred, low, last))
            both_weights(*targets, *sources, buf, j)

    def self_second(group, buf):
        low, last = rows_of()
        for j in range(UNROLL):
            leaf = group * UNROLL + j
            block = pool[leaf]
            centred, mass = centre(block, last), block[3:4, :]
            mom = moments(centred, low, last, mass)
            moment_o[leaf] = mom
            f = force(folded(dot(mom, buf[j])), centred, mass)
            for c in range(3):
                self_f[c, pl.ds(leaf, 1), :] = f[c : c + 1, :]

    bufs = (buf0, buf1)
    pipeline(leaves // UNROLL, self_first, self_second, bufs)

    for role, copy in enumerate(ahead):
        copy.wait_recv()
        a = 2 * role - 1
        slot = slot_of(a, 0)
        out_copies.append(export(6 + role, 0, inner, (outer + 1) if a < 0 else (outer + 6), ghosts_at(slot)))
    for copy in out_copies:
        copy.wait_recv()

    def pair_first(group, buf):
        low, last = rows_of()
        for j in range(0, UNROLL, 2):
            targets, sources = [], []
            for p in (group * UNROLL + j, group * UNROLL + j + 1):
                targets.append(target_t[pairs_s[0, 0, p]])
                centred = centre(pool[pairs_s[1, 0, p]], last)
                sources.append(source_features(centred, low, last))
            both_weights(*targets, *sources, buf, j)

    def pair_second(group, buf):
        low, last = rows_of()
        for j in range(UNROLL):
            p = group * UNROLL + j
            target, source = pairs_s[0, 0, p], pairs_s[1, 0, p]
            t_block, s_block = pool[target], pool[source]
            t_centred, t_mass = centre(t_block, last), t_block[3:4, :]
            s_centred, s_mass = centre(s_block, last), s_block[3:4, :]
            s_mom = moments(s_centred, low, last, s_mass)
            s_mom = jnp.concatenate([s_mom, s_mom], axis=1)
            on_target = force(dot_t(s_mom, buf[j]), t_centred, t_mass)
            on_source = force(folded(dot(moment_o[target], buf[j])), s_centred, s_mass)
            for c in range(3):
                pair_f[c, pl.ds(p, 1), :] = on_target[c : c + 1, :]
                pair_f[c, pl.ds(pair_slots + p, 1), :] = on_source[c : c + 1, :]

    pipeline(pair_slots // UNROLL, pair_first, pair_second, bufs)

    key = jnp.concatenate([pairs_v[0], pairs_v[1]], axis=1)
    slot = lax.broadcasted_iota(jnp.int32, (1, 2 * pair_slots), 1)
    slot = jnp.where(slot < pair_slots, slot, slot - pair_slots)
    key = jnp.where(slot < pcount_s[0, 0], key, -1)
    key = jnp.concatenate([key, key], axis=1)

    def two(x):
        h = x.astype(BF16)
        return jnp.concatenate([h, (x - h.astype(F32)).astype(BF16)], axis=0)

    results = two(jnp.concatenate([pair_f[0], pair_f[1], pair_f[2]], axis=1))

    def scatter(starts, rows):
        index = lax.broadcasted_iota(jnp.int32, (rows, 4 * pair_slots), 0)
        pick = [jnp.where(index + start == key, 1.0, 0.0) for start in starts]
        return dot(jnp.concatenate(pick, axis=0).astype(BF16), results)

    order = [inner + 1, inner + 6, 3 + (inner + 1) // 2]
    order += [outer + 1, outer + 6, 3 + (outer + 1) // 2, slot_of(-1, 0), slot_of(1, 0)]
    ghosts = scatter([leaves + slot * g_total for slot in order], g_total)
    for k in range(8):
        for c in range(3):
            ghost_f[k, c] = ghosts[k * g_total : (k + 1) * g_total, c * 128 : (c + 1) * 128]

    def back(role, a, b, src, dst):
        return remote(src, dst, send2_sem, recv2_sem, role, a, b)

    vias = [back(0, 0, inner, ghost_f.at[0], via.at[0]), back(1, 0, inner, ghost_f.at[1], via.at[1])]
    returns = [
        back(3, -1, outer, ghost_f.at[3], returned.at[1]),
        back(4, 1, outer, ghost_f.at[4], returned.at[2]),
        back(5, 0, outer, ghost_f.at[5], returned.at[3]),
        back(2, 0, inner, ghost_f.at[2], returned.at[0]),
    ]
    for i, copy in enumerate(vias):
        copy.wait_recv()
        passed[i] = ghost_f[6 + i] + via[i]
        returns.append(back(6 + i, 2 * i - 1, 0, passed.at[i], returned.at[4 + i]))

    mine = scatter([0], leaves)
    for c in range(3):
        acc[c] = mine[:, c * 128 : (c + 1) * 128] + self_f[c]
    for copy in ahead + out_copies + vias:
        copy.wait_send()
    slots2 = jnp.concatenate([slots_v[...], slots_v[...]], axis=1)
    index = lax.broadcasted_iota(jnp.int32, (leaves, 2 * g_total), 0)
    pick = jnp.where(index == slots2, 1.0, 0.0).astype(BF16)
    for copy in returns:
        copy.wait_recv()
    for c in range(3):
        total = returned[0, c]
        for k in range(1, 6):
            total = total + returned[k, c]
        out_ref[c, 0] = acc[c] + dot(pick, two(total))
    for copy in returns:
        copy.wait_send()


def local(shape, positions, masses, occupancy, export_slots, export_count, pair_list, pair_count):
    leaves, width = masses.shape[1:]
    g_total = export_slots.shape[1]
    pair_slots = pair_list.shape[2]
    far = pl.BlockSpec(memory_space=pltpu.HBM)
    return pl.pallas_call(
        functools.partial(kernel, shape),
        out_shape=pltpu.VMEM(positions.shape, F32),
        in_specs=[far] * 7,
        out_specs=pl.BlockSpec(memory_space=pltpu.VMEM),
        scratch_shapes=[
            pltpu.VMEM((3, leaves, width), F32),
            pltpu.VMEM((leaves, width), F32),
            pltpu.SMEM((1, leaves), jnp.int32),
            pltpu.SMEM((1, g_total), jnp.int32),
            pltpu.SMEM((1, 1), jnp.int32),
            pltpu.SMEM((2, 1, pair_slots), jnp.int32),
            pltpu.SMEM((1, 1), jnp.int32),
            pltpu.VMEM((1, g_total), jnp.int32),
            pltpu.VMEM((2, 1, pair_slots), jnp.int32),
            pltpu.VMEM((g_total, 4, width), F32),
            pltpu.VMEM((leaves + 8 * g_total, 4, width), F32),
            pltpu.VMEM((leaves, width, 64), BF16),
            pltpu.VMEM((leaves, 16, width), BF16),
            pltpu.VMEM((UNROLL, width, 2 * width), BF16),
            pltpu.VMEM((UNROLL, width, 2 * width), BF16),
            pltpu.VMEM((3, leaves, width), F32),
            pltpu.VMEM((3, 2 * pair_slots, width), F32),
            pltpu.VMEM((8, 3, g_total, width), F32),
            pltpu.VMEM((2, 3, g_total, width), F32),
            pltpu.VMEM((2, 3, g_total, width), F32),
            pltpu.VMEM((6, 3, g_total, width), F32),
            pltpu.VMEM((3, leaves, width), F32),
            pltpu.SemaphoreType.DMA((9,)),
            pltpu.SemaphoreType.DMA((8,)),
            pltpu.SemaphoreType.DMA((8,)),
            pltpu.SemaphoreType.DMA((8,)),
            pltpu.SemaphoreType.DMA((8,)),
        ],
        compiler_params=pltpu.CompilerParams(collective_id=0, has_side_effects=True),
    )(positions, masses, occupancy, export_slots, export_count, pair_list, pair_count)


def solution(mesh):
    return jax.shard_map(
        functools.partial(local, (mesh.shape["space"], mesh.shape["sub"])),
        mesh=mesh,
        in_specs=(
            P(None, "space", "sub", None),
            P("space", "sub", None),
            P("space", "sub"),
            P("space", "sub"),
            P("space", "sub"),
            P(None, "space", "sub"),
            P("space", "sub"),
        ),
        out_specs=P(None, "space", "sub", None),
        check_vma=False,
    )
```

```python
import functools

import jax
import jax.numpy as jnp
from jax import lax
from jax.experimental import pallas as pl
from jax.experimental.pallas import tpu as pltpu
from jax.sharding import PartitionSpec as P

OFFSETS = ((-1, -1), (-1, 0), (-1, 1), (0, -1), (0, 1), (1, -1), (1, 0), (1, 1))
SOFTEN = 0.05
CENTRE = 0.75
MESH = pl.DeviceIdType.MESH
F32 = jnp.float32
BF16 = jnp.bfloat16
UNROLL = 4


def split3(x):
    h = x.astype(BF16).astype(F32)
    rest = x - h
    m = rest.astype(BF16).astype(F32)
    return h, m, rest - m


def masks():
    row = lax.broadcasted_iota(jnp.int32, (8, 128), 0)
    return row < 4, (row == 3) | (row == 7)


def two_leaves(first, second, low, last):
    both = jnp.concatenate([first, second], axis=0)
    mass = jnp.where(low, both[3:4, :], both[7:8, :])
    return jnp.where(last, 0.0, both - CENTRE), mass


def swap(x):
    return pltpu.roll(x, 4, 0)


def squared(centred, last, extra):
    t = centred * centred
    t = t + pltpu.roll(t, 1, 0)
    t = t + pltpu.roll(t, 2, 0) + extra
    return split3(jnp.where(last, t, centred))


def halves(low, upper, lower):
    return jnp.where(low, upper, swap(lower)), jnp.where(low, swap(upper), lower)


def stacked(low, blocks):
    parts = [halves(low, upper, lower) for upper, lower in blocks]
    zero = jnp.zeros((8, 128), F32)
    pad = [zero] * (4 - len(parts)) if len(parts) > 2 else []
    return [jnp.concatenate([p[i] for p in parts] + pad, axis=0).astype(BF16) for i in range(2)]


def target_features(centred, low, last):
    h, m, l = squared(centred, last, 0.0)
    h1 = jnp.where(last, 1.0, h)
    m1 = jnp.where(last, 1.0, m)
    return stacked(low, [(h, m), (l, h1), (h1, m1)])


def source_features(centred, low, last):
    h, m, l = squared(centred, last, SOFTEN)
    head = jnp.where(last, 1.0, -2.0 * h)
    minus = -2.0 * m
    return stacked(
        low,
        [
            (head, head),
            (head, jnp.where(last, h, minus)),
            (jnp.where(last, m, -2.0 * l), jnp.where(last, l, minus)),
        ],
    )


def moments(centred, mass, low, last):
    h, m, l = split3(jnp.where(last, 1.0, centred) * mass)
    return stacked(low, [(h, m), (l, jnp.zeros_like(l))])


def weights(softened):
    falloff = jnp.maximum((1.0 + SOFTEN) - softened, 0.0)
    root = lax.rsqrt(softened)
    scaled = falloff * root
    return scaled * scaled * root


def force(first, second, centred, mass, low):
    a, b = (t[0:8, 0:128] + t[0:8, 128:256] + (t[8:16, 0:128] + t[8:16, 128:256]) for t in (first, second))
    both = jnp.where(low, a, b) + swap(jnp.where(low, b, a))
    return mass * (both - centred * jnp.where(low, both[3:4, :], both[7:8, :]))


def dot(a, b):
    return jnp.dot(a, b, preferred_element_type=F32)


def distances(targets, sources):
    zero = jnp.zeros_like(sources[0])
    source = jnp.concatenate(
        [
            jnp.concatenate([sources[0], zero], axis=1),
            jnp.concatenate([zero, sources[1]], axis=1),
        ],
        axis=0,
    )
    return dot(jnp.concatenate(targets, axis=0).T, source)


def weigh(dist, buf):
    for j in range(UNROLL):
        w = weights(dist[j])
        buf[0, j] = w.astype(BF16)
        buf[1, j] = (w - buf[0, j].astype(F32)).astype(BF16)


def beside(buf, j):
    return jnp.concatenate([buf[0, j], buf[1, j]], axis=1)


def turned(buf, j):
    return jnp.concatenate([buf[0, j].T, buf[1, j].T], axis=1)


def pipeline(groups, measure, combine, dists, bufs):
    measure(0, dists[0])
    weigh(dists[0], bufs[0])
    measure(1, dists[1])

    def step(i, carry):
        combine(2 * i, bufs[0])
        weigh(dists[1], bufs[1])
        measure(2 * i + 2, dists[0])
        combine(2 * i + 1, bufs[1])
        weigh(dists[0], bufs[0])
        measure(2 * i + 3, dists[1])
        return carry

    lax.fori_loop(0, groups // 2 - 1, step, 0)
    combine(groups - 2, bufs[0])
    weigh(dists[1], bufs[1])
    combine(groups - 1, bufs[1])


def slot_of(a, b):
    if a == 0:
        return 3 + (b + 1) // 2
    return b + 1 if a < 0 else b + 6


def kernel(
    shape,
    pos_hbm, mass_hbm, occ_hbm, slots_hbm, ecount_hbm, pairs_hbm, pcount_hbm,
    out_ref,
    pos_v, mass_v, occ_s, slots_s, ecount_s, pairs_s, pcount_s, slots_v, pairs_v,
    sent, pool, target_o, moment_o, dist0, dist1, buf0, buf1, self_f, pair_f, ghost_f, via, passed, returned, acc,
    in_sem, send_sem, recv_sem, send2_sem, recv2_sem,
):
    n_space, n_sub = shape
    leaves = pos_v.shape[1]
    g_total = sent.shape[0]
    pair_slots = pairs_v.shape[2]
    s = lax.axis_index("space")
    r = lax.axis_index("sub")
    inner = 1 - 2 * lax.rem(r, 2)
    outer = -inner

    def place(a, b):
        return (lax.rem(s + a + n_space, n_space), lax.rem(r + b + n_sub, n_sub))

    loads = [
        pltpu.make_async_copy(src, dst, in_sem.at[i])
        for i, (src, dst) in enumerate(
            [
                (slots_hbm, slots_s),
                (occ_hbm, occ_s),
                (ecount_hbm, ecount_s),
                (pcount_hbm, pcount_s),
                (pos_hbm.at[:, 0], pos_v),
                (mass_hbm.at[0], mass_v),
                (pairs_hbm, pairs_s),
                (slots_hbm, slots_v),
                (pairs_hbm, pairs_v),
            ]
        )
    ]
    for load in loads:
        load.start()
    barrier = pltpu.get_barrier_semaphore()
    for a, b in OFFSETS:
        pl.semaphore_signal(barrier, inc=1, device_id=place(a, b), device_id_type=MESH)
    for load in loads:
        load.wait()

    lane = lax.broadcasted_iota(jnp.int32, (1, 128), 1)
    exported = ecount_s[0, 0]

    def gather(i, carry):
        for j in range(8):
            g = i * 8 + j
            slot = slots_s[0, g]
            for c in range(3):
                sent[g, pl.ds(c, 1), :] = pos_v[c, pl.ds(slot, 1), :]
            live = jnp.where(g < exported, occ_s[0, slot], 0)
            sent[g, pl.ds(3, 1), :] = jnp.where(lane < live, mass_v[pl.ds(slot, 1), :], 0.0)
        return carry

    lax.fori_loop(0, g_total // 8, gather, 0)
    pl.semaphore_wait(barrier, len(OFFSETS))

    def remote(src, dst, send, recv, role, a, b):
        copy = pltpu.make_async_remote_copy(
            src_ref=src,
            dst_ref=dst,
            send_sem=send.at[role],
            recv_sem=recv.at[role],
            device_id=place(a, b),
            device_id_type=MESH,
        )
        copy.start()
        return copy

    def ghosts_at(slot):
        return pool.at[pl.ds(leaves + slot * g_total, g_total)]

    def export(role, a, b, slot, src=sent):
        return remote(src, ghosts_at(slot), send_sem, recv_sem, role, a, b)

    ahead = [export(0, 1, 0, slot_of(-1, 0)), export(1, -1, 0, slot_of(1, 0))]
    out_copies = [
        export(4, 1, outer, inner + 1),
        export(5, -1, outer, inner + 6),
        export(3, 0, outer, 3 + (inner + 1) // 2),
        export(2, 0, inner, 3 + (outer + 1) // 2),
    ]

    def own(i, carry):
        for j in range(8):
            leaf = i * 8 + j
            for c in range(3):
                pool[leaf, pl.ds(c, 1), :] = pos_v[c, pl.ds(leaf, 1), :]
            pool[leaf, pl.ds(3, 1), :] = jnp.where(
                lane < occ_s[0, leaf], mass_v[pl.ds(leaf, 1), :], 0.0
            )
        return carry

    lax.fori_loop(0, leaves // 8, own, 0)

    def rows_at(i):
        return pl.ds(pl.multiple_of(8 * i, 8), 8)

    def self_measure(group, dist):
        low, last = masks()
        for j in range(0, UNROLL, 2):
            leaf = group * UNROLL + j
            centred, mass = two_leaves(pool[leaf], pool[leaf + 1], low, last)
            targets = target_features(centred, low, last)
            both = distances(targets, source_features(centred, low, last))
            mom = moments(centred, mass, low, last)
            for i in range(2):
                dist[j + i] = both[:, i * 128 : (i + 1) * 128]
                target_o[leaf + i] = targets[i]
                moment_o[leaf + i] = mom[i]

    def self_combine(group, buf):
        low, last = masks()
        for j in range(0, UNROLL, 2):
            leaf = group * UNROLL + j
            centred, mass = two_leaves(pool[leaf], pool[leaf + 1], low, last)
            sums = [dot(moment_o[leaf + i], beside(buf, j + i)) for i in range(2)]
            self_f[rows_at(group * (UNROLL // 2) + j // 2), :] = force(*sums, centred, mass, low)

    stages = ((dist0, dist1), (buf0, buf1))
    pipeline(leaves // UNROLL, self_measure, self_combine, *stages)

    for role, copy in enumerate(ahead):
        copy.wait_recv()
        a = 2 * role - 1
        slot = slot_of(a, 0)
        out_copies.append(export(6 + role, 0, inner, (outer + 1) if a < 0 else (outer + 6), ghosts_at(slot)))
    for copy in out_copies:
        copy.wait_recv()

    def pair_measure(group, dist):
        low, last = masks()
        for j in range(0, UNROLL, 2):
            p = group * UNROLL + j
            centred, mass = two_leaves(pool[pairs_s[1, 0, p]], pool[pairs_s[1, 0, p + 1]], low, last)
            targets = [target_o[pairs_s[0, 0, p]], target_o[pairs_s[0, 0, p + 1]]]
            both = distances(targets, source_features(centred, low, last))
            for i in range(2):
                dist[j + i] = both[:, i * 128 : (i + 1) * 128]

    def pair_combine(group, buf):
        low, last = masks()
        for j in range(0, UNROLL, 2):
            p = group * UNROLL + j
            at = group * (UNROLL // 2) + j // 2
            targets = [pairs_s[0, 0, p], pairs_s[0, 0, p + 1]]
            t_centred, t_mass = two_leaves(*[pool[t] for t in targets], low, last)
            centred, mass = two_leaves(pool[pairs_s[1, 0, p]], pool[pairs_s[1, 0, p + 1]], low, last)
            mom = moments(centred, mass, low, last)
            sums = [dot(moment_o[targets[i]], beside(buf, j + i)) for i in range(2)]
            pair_f[rows_at(pair_slots // 2 + at), :] = force(*sums, centred, mass, low)
            sums = [dot(mom[i], turned(buf, j + i)) for i in range(2)]
            pair_f[rows_at(at), :] = force(*sums, t_centred, t_mass, low)

    pipeline(pair_slots // UNROLL, pair_measure, pair_combine, *stages)

    key = jnp.concatenate([pairs_v[0], pairs_v[1]], axis=1)
    slot = lax.broadcasted_iota(jnp.int32, (1, 2 * pair_slots), 1)
    slot = jnp.where(slot < pair_slots, slot, slot - pair_slots)
    key = jnp.where(slot < pcount_s[0, 0], key, -1)
    key = jnp.concatenate([key, key], axis=1)

    def two(x):
        h = x.astype(BF16)
        return jnp.concatenate([h, (x - h.astype(F32)).astype(BF16)], axis=0)

    results = two(
        jnp.concatenate([pair_f[pl.ds(c, 2 * pair_slots, stride=4), :] for c in range(3)], axis=1)
    )

    def scatter(starts, rows):
        index = lax.broadcasted_iota(jnp.int32, (rows, 4 * pair_slots), 0)
        pick = [jnp.where(index + start == key, 1.0, 0.0) for start in starts]
        return dot(jnp.concatenate(pick, axis=0).astype(BF16), results)

    order = [inner + 1, inner + 6, 3 + (inner + 1) // 2]
    order += [outer + 1, outer + 6, 3 + (outer + 1) // 2, slot_of(-1, 0), slot_of(1, 0)]
    ghosts = scatter([leaves + slot * g_total for slot in order], g_total)
    for k in range(8):
        for c in range(3):
            ghost_f[k, c] = ghosts[k * g_total : (k + 1) * g_total, c * 128 : (c + 1) * 128]

    def back(role, a, b, src, dst):
        return remote(src, dst, send2_sem, recv2_sem, role, a, b)

    vias = [back(0, 0, inner, ghost_f.at[0], via.at[0]), back(1, 0, inner, ghost_f.at[1], via.at[1])]
    returns = [
        back(3, -1, outer, ghost_f.at[3], returned.at[1]),
        back(4, 1, outer, ghost_f.at[4], returned.at[2]),
        back(5, 0, outer, ghost_f.at[5], returned.at[3]),
        back(2, 0, inner, ghost_f.at[2], returned.at[0]),
    ]
    for i, copy in enumerate(vias):
        copy.wait_recv()
        passed[i] = ghost_f[6 + i] + via[i]
        returns.append(back(6 + i, 2 * i - 1, 0, passed.at[i], returned.at[4 + i]))

    mine = scatter([0], leaves)
    for c in range(3):
        acc[c] = mine[:, c * 128 : (c + 1) * 128] + self_f[pl.ds(c, leaves, stride=4), :]
    for copy in ahead + out_copies + vias:
        copy.wait_send()
    slots2 = jnp.concatenate([slots_v[...], slots_v[...]], axis=1)
    index = lax.broadcasted_iota(jnp.int32, (leaves, 2 * g_total), 0)
    pick = jnp.where(index == slots2, 1.0, 0.0).astype(BF16)
    for copy in returns:
        copy.wait_recv()
    for c in range(3):
        total = returned[0, c]
        for k in range(1, 6):
            total = total + returned[k, c]
        out_ref[c, 0] = acc[c] + dot(pick, two(total))
    for copy in returns:
        copy.wait_send()


def local(shape, positions, masses, occupancy, export_slots, export_count, pair_list, pair_count):
    leaves, width = masses.shape[1:]
    g_total = export_slots.shape[1]
    pair_slots = pair_list.shape[2]
    far = pl.BlockSpec(memory_space=pltpu.HBM)
    return pl.pallas_call(
        functools.partial(kernel, shape),
        out_shape=pltpu.VMEM(positions.shape, F32),
        in_specs=[far] * 7,
        out_specs=pl.BlockSpec(memory_space=pltpu.VMEM),
        scratch_shapes=[
            pltpu.VMEM((3, leaves, width), F32),
            pltpu.VMEM((leaves, width), F32),
            pltpu.SMEM((1, leaves), jnp.int32),
            pltpu.SMEM((1, g_total), jnp.int32),
            pltpu.SMEM((1, 1), jnp.int32),
            pltpu.SMEM((2, 1, pair_slots), jnp.int32),
            pltpu.SMEM((1, 1), jnp.int32),
            pltpu.VMEM((1, g_total), jnp.int32),
            pltpu.VMEM((2, 1, pair_slots), jnp.int32),
            pltpu.VMEM((g_total, 4, width), F32),
            pltpu.VMEM((leaves + 8 * g_total, 4, width), F32),
            pltpu.VMEM((leaves, 32, width), BF16),
            pltpu.VMEM((leaves, 16, width), BF16),
            pltpu.VMEM((UNROLL, width, width), F32),
            pltpu.VMEM((UNROLL, width, width), F32),
            pltpu.VMEM((2, UNROLL, width, width), BF16),
            pltpu.VMEM((2, UNROLL, width, width), BF16),
            pltpu.VMEM((4 * leaves, width), F32),
            pltpu.VMEM((8 * pair_slots, width), F32),
            pltpu.VMEM((8, 3, g_total, width), F32),
            pltpu.VMEM((2, 3, g_total, width), F32),
            pltpu.VMEM((2, 3, g_total, width), F32),
            pltpu.VMEM((6, 3, g_total, width), F32),
            pltpu.VMEM((3, leaves, width), F32),
            pltpu.SemaphoreType.DMA((9,)),
            pltpu.SemaphoreType.DMA((8,)),
            pltpu.SemaphoreType.DMA((8,)),
            pltpu.SemaphoreType.DMA((8,)),
            pltpu.SemaphoreType.DMA((8,)),
        ],
        compiler_params=pltpu.CompilerParams(collective_id=0, has_side_effects=True),
    )(positions, masses, occupancy, export_slots, export_count, pair_list, pair_count)


def solution(mesh):
    return jax.shard_map(
        functools.partial(local, (mesh.shape["space"], mesh.shape["sub"])),
        mesh=mesh,
        in_specs=(
            P(None, "space", "sub", None),
            P("space", "sub", None),
            P("space", "sub"),
            P("space", "sub"),
            P("space", "sub"),
            P(None, "space", "sub"),
            P("space", "sub"),
        ),
        out_specs=P(None, "space", "sub", None),
        check_vma=False,
    )
```

```python
import functools

import jax
import jax.numpy as jnp
from jax import lax
from jax.experimental import pallas as pl
from jax.experimental.pallas import tpu as pltpu
from jax.sharding import PartitionSpec as P

OFFSETS = ((-1, -1), (-1, 0), (-1, 1), (0, -1), (0, 1), (1, -1), (1, 0), (1, 1))
SOFTEN = 0.05
CENTRE = 0.75
MESH = pl.DeviceIdType.MESH
F32 = jnp.float32
BF16 = jnp.bfloat16
UNROLL = 8


def split3(x):
    h = x.astype(BF16).astype(F32)
    rest = x - h
    m = rest.astype(BF16).astype(F32)
    return h, m, rest - m


def masks():
    row = lax.broadcasted_iota(jnp.int32, (8, 128), 0)
    return row < 4, (row == 3) | (row == 7)


def two_leaves(first, second, low, last):
    both = jnp.concatenate([first, second], axis=0)
    mass = jnp.where(low, both[3:4, :], both[7:8, :])
    return jnp.where(last, 0.0, both - CENTRE), mass


def swap(x):
    return pltpu.roll(x, 4, 0)


def squared(centred, last, extra):
    t = centred * centred
    t = t + pltpu.roll(t, 1, 0)
    t = t + pltpu.roll(t, 2, 0) + extra
    return split3(jnp.where(last, t, centred))


def halves(low, upper, lower):
    return jnp.where(low, upper, swap(lower)), jnp.where(low, swap(upper), lower)


def stacked(low, blocks):
    parts = [halves(low, upper, lower) for upper, lower in blocks]
    zero = jnp.zeros((8, 128), F32)
    pad = [zero] * (4 - len(parts)) if len(parts) > 2 else []
    return [jnp.concatenate([p[i] for p in parts] + pad, axis=0).astype(BF16) for i in range(2)]


def target_features(centred, low, last):
    h, m, l = squared(centred, last, 0.0)
    h1 = jnp.where(last, 1.0, h)
    m1 = jnp.where(last, 1.0, m)
    return stacked(low, [(h, m), (l, h1), (h1, m1)])


def source_features(centred, low, last):
    h, m, l = squared(centred, last, SOFTEN)
    head = jnp.where(last, 1.0, -2.0 * h)
    minus = -2.0 * m
    return stacked(
        low,
        [
            (head, head),
            (head, jnp.where(last, h, minus)),
            (jnp.where(last, m, -2.0 * l), jnp.where(last, l, minus)),
        ],
    )


def moments(centred, mass, low, last):
    h, m, l = split3(jnp.where(last, 1.0, centred) * mass)
    return stacked(low, [(h, m), (l, jnp.zeros_like(l))])


def weights(softened):
    falloff = jnp.maximum((1.0 + SOFTEN) - softened, 0.0)
    root = lax.rsqrt(softened)
    scaled = falloff * root
    return scaled * scaled * root


def force(first, second, centred, mass, low):
    a, b = (t[0:8, 0:128] + t[0:8, 128:256] + (t[8:16, 0:128] + t[8:16, 128:256]) for t in (first, second))
    both = jnp.where(low, a, b) + swap(jnp.where(low, b, a))
    return mass * (both - centred * jnp.where(low, both[3:4, :], both[7:8, :]))


def dot(a, b):
    return jnp.dot(a, b, preferred_element_type=F32)


def distances(targets, sources):
    zero = jnp.zeros_like(sources[0])
    source = jnp.concatenate(
        [
            jnp.concatenate([sources[0], zero], axis=1),
            jnp.concatenate([zero, sources[1]], axis=1),
        ],
        axis=0,
    )
    return dot(jnp.concatenate(targets, axis=0).T, source)


def weigh(dist, buf):
    for j in range(UNROLL):
        w = weights(dist[j])
        buf[0, j] = w.astype(BF16)
        buf[1, j] = (w - buf[0, j].astype(F32)).astype(BF16)


def beside(buf, j):
    return jnp.concatenate([buf[0, j], buf[1, j]], axis=1)


def turned(buf, j):
    return jnp.concatenate([buf[0, j].T, buf[1, j].T], axis=1)


def pipeline(groups, measure, combine, dists, bufs):
    measure(0, dists[0])
    weigh(dists[0], bufs[0])
    measure(1, dists[1])

    def step(i, carry):
        combine(2 * i, bufs[0])
        weigh(dists[1], bufs[1])
        measure(2 * i + 2, dists[0])
        combine(2 * i + 1, bufs[1])
        weigh(dists[0], bufs[0])
        measure(2 * i + 3, dists[1])
        return carry

    lax.fori_loop(0, groups // 2 - 1, step, 0)
    combine(groups - 2, bufs[0])
    weigh(dists[1], bufs[1])
    combine(groups - 1, bufs[1])


def slot_of(a, b):
    if a == 0:
        return 3 + (b + 1) // 2
    return b + 1 if a < 0 else b + 6


def kernel(
    shape,
    pos_hbm, mass_hbm, occ_hbm, slots_hbm, ecount_hbm, pairs_hbm, pcount_hbm,
    out_ref,
    pos_v, mass_v, occ_s, slots_s, ecount_s, pairs_s, pcount_s, slots_v, pairs_v,
    sent, pool, target_o, moment_o, dist0, dist1, buf0, buf1, self_f, pair_f, ghost_f, via, passed, returned, acc,
    in_sem, send_sem, recv_sem, send2_sem, recv2_sem,
):
    n_space, n_sub = shape
    leaves = pos_v.shape[1]
    g_total = sent.shape[0]
    pair_slots = pairs_v.shape[2]
    s = lax.axis_index("space")
    r = lax.axis_index("sub")
    inner = 1 - 2 * lax.rem(r, 2)
    outer = -inner

    def place(a, b):
        return (lax.rem(s + a + n_space, n_space), lax.rem(r + b + n_sub, n_sub))

    loads = [
        pltpu.make_async_copy(src, dst, in_sem.at[i])
        for i, (src, dst) in enumerate(
            [
                (slots_hbm, slots_s),
                (occ_hbm, occ_s),
                (ecount_hbm, ecount_s),
                (pcount_hbm, pcount_s),
                (pos_hbm.at[:, 0], pos_v),
                (mass_hbm.at[0], mass_v),
                (pairs_hbm, pairs_s),
                (slots_hbm, slots_v),
                (pairs_hbm, pairs_v),
            ]
        )
    ]
    for load in loads:
        load.start()
    barrier = pltpu.get_barrier_semaphore()
    for a, b in OFFSETS:
        pl.semaphore_signal(barrier, inc=1, device_id=place(a, b), device_id_type=MESH)
    for load in loads:
        load.wait()

    lane = lax.broadcasted_iota(jnp.int32, (1, 128), 1)
    exported = ecount_s[0, 0]

    def gather(i, carry):
        for j in range(8):
            g = i * 8 + j
            slot = slots_s[0, g]
            for c in range(3):
                sent[g, pl.ds(c, 1), :] = pos_v[c, pl.ds(slot, 1), :]
            live = jnp.where(g < exported, occ_s[0, slot], 0)
            sent[g, pl.ds(3, 1), :] = jnp.where(lane < live, mass_v[pl.ds(slot, 1), :], 0.0)
        return carry

    lax.fori_loop(0, g_total // 8, gather, 0)
    pl.semaphore_wait(barrier, len(OFFSETS))

    def remote(src, dst, send, recv, role, a, b):
        copy = pltpu.make_async_remote_copy(
            src_ref=src,
            dst_ref=dst,
            send_sem=send.at[role],
            recv_sem=recv.at[role],
            device_id=place(a, b),
            device_id_type=MESH,
        )
        copy.start()
        return copy

    def ghosts_at(slot):
        return pool.at[pl.ds(leaves + slot * g_total, g_total)]

    def export(role, a, b, slot, src=sent):
        return remote(src, ghosts_at(slot), send_sem, recv_sem, role, a, b)

    ahead = [export(0, 1, 0, slot_of(-1, 0)), export(1, -1, 0, slot_of(1, 0))]
    out_copies = [
        export(4, 1, outer, inner + 1),
        export(5, -1, outer, inner + 6),
        export(3, 0, outer, 3 + (inner + 1) // 2),
        export(2, 0, inner, 3 + (outer + 1) // 2),
    ]

    def own(i, carry):
        for j in range(8):
            leaf = i * 8 + j
            for c in range(3):
                pool[leaf, pl.ds(c, 1), :] = pos_v[c, pl.ds(leaf, 1), :]
            pool[leaf, pl.ds(3, 1), :] = jnp.where(
                lane < occ_s[0, leaf], mass_v[pl.ds(leaf, 1), :], 0.0
            )
        return carry

    lax.fori_loop(0, leaves // 8, own, 0)

    def rows_at(i):
        return pl.ds(pl.multiple_of(8 * i, 8), 8)

    def self_measure(group, dist):
        low, last = masks()
        for j in range(0, UNROLL, 2):
            leaf = group * UNROLL + j
            centred, mass = two_leaves(pool[leaf], pool[leaf + 1], low, last)
            targets = target_features(centred, low, last)
            both = distances(targets, source_features(centred, low, last))
            mom = moments(centred, mass, low, last)
            for i in range(2):
                dist[j + i] = both[:, i * 128 : (i + 1) * 128]
                target_o[leaf + i] = targets[i]
                moment_o[leaf + i] = mom[i]

    def self_combine(group, buf):
        low, last = masks()
        for j in range(0, UNROLL, 2):
            leaf = group * UNROLL + j
            centred, mass = two_leaves(pool[leaf], pool[leaf + 1], low, last)
            sums = [dot(moment_o[leaf + i], beside(buf, j + i)) for i in range(2)]
            self_f[rows_at(group * (UNROLL // 2) + j // 2), :] = force(*sums, centred, mass, low)

    stages = ((dist0, dist1), (buf0, buf1))
    pipeline(leaves // UNROLL, self_measure, self_combine, *stages)

    for role, copy in enumerate(ahead):
        copy.wait_recv()
        a = 2 * role - 1
        slot = slot_of(a, 0)
        out_copies.append(export(6 + role, 0, inner, (outer + 1) if a < 0 else (outer + 6), ghosts_at(slot)))
    for copy in out_copies:
        copy.wait_recv()

    def pair_measure(group, dist):
        low, last = masks()
        for j in range(0, UNROLL, 2):
            p = group * UNROLL + j
            centred, mass = two_leaves(pool[pairs_s[1, 0, p]], pool[pairs_s[1, 0, p + 1]], low, last)
            targets = [target_o[pairs_s[0, 0, p]], target_o[pairs_s[0, 0, p + 1]]]
            both = distances(targets, source_features(centred, low, last))
            for i in range(2):
                dist[j + i] = both[:, i * 128 : (i + 1) * 128]

    def pair_combine(group, buf):
        low, last = masks()
        for j in range(0, UNROLL, 2):
            p = group * UNROLL + j
            at = group * (UNROLL // 2) + j // 2
            targets = [pairs_s[0, 0, p], pairs_s[0, 0, p + 1]]
            t_centred, t_mass = two_leaves(*[pool[t] for t in targets], low, last)
            centred, mass = two_leaves(pool[pairs_s[1, 0, p]], pool[pairs_s[1, 0, p + 1]], low, last)
            mom = moments(centred, mass, low, last)
            sums = [dot(moment_o[targets[i]], beside(buf, j + i)) for i in range(2)]
            pair_f[rows_at(pair_slots // 2 + at), :] = force(*sums, centred, mass, low)
            sums = [dot(mom[i], turned(buf, j + i)) for i in range(2)]
            pair_f[rows_at(at), :] = force(*sums, t_centred, t_mass, low)

    pipeline(pair_slots // UNROLL, pair_measure, pair_combine, *stages)

    key = jnp.concatenate([pairs_v[0], pairs_v[1]], axis=1)
    slot = lax.broadcasted_iota(jnp.int32, (1, 2 * pair_slots), 1)
    slot = jnp.where(slot < pair_slots, slot, slot - pair_slots)
    key = jnp.where(slot < pcount_s[0, 0], key, -1)
    key = jnp.concatenate([key, key], axis=1)

    def two(x):
        h = x.astype(BF16)
        return jnp.concatenate([h, (x - h.astype(F32)).astype(BF16)], axis=0)

    results = two(
        jnp.concatenate([pair_f[pl.ds(c, 2 * pair_slots, stride=4), :] for c in range(3)], axis=1)
    )

    def scatter(starts, rows):
        index = lax.broadcasted_iota(jnp.int32, (rows, 4 * pair_slots), 0)
        pick = [jnp.where(index + start == key, 1.0, 0.0) for start in starts]
        return dot(jnp.concatenate(pick, axis=0).astype(BF16), results)

    order = [inner + 1, inner + 6, 3 + (inner + 1) // 2]
    order += [outer + 1, outer + 6, 3 + (outer + 1) // 2, slot_of(-1, 0), slot_of(1, 0)]
    ghosts = scatter([leaves + slot * g_total for slot in order], g_total)
    for k in range(8):
        for c in range(3):
            ghost_f[k, c] = ghosts[k * g_total : (k + 1) * g_total, c * 128 : (c + 1) * 128]

    def back(role, a, b, src, dst):
        return remote(src, dst, send2_sem, recv2_sem, role, a, b)

    vias = [back(0, 0, inner, ghost_f.at[0], via.at[0]), back(1, 0, inner, ghost_f.at[1], via.at[1])]
    returns = [
        back(3, -1, outer, ghost_f.at[3], returned.at[1]),
        back(4, 1, outer, ghost_f.at[4], returned.at[2]),
        back(5, 0, outer, ghost_f.at[5], returned.at[3]),
        back(2, 0, inner, ghost_f.at[2], returned.at[0]),
    ]
    for i, copy in enumerate(vias):
        copy.wait_recv()
        passed[i] = ghost_f[6 + i] + via[i]
        returns.append(back(6 + i, 2 * i - 1, 0, passed.at[i], returned.at[4 + i]))

    mine = scatter([0], leaves)
    for c in range(3):
        acc[c] = mine[:, c * 128 : (c + 1) * 128] + self_f[pl.ds(c, leaves, stride=4), :]
    for copy in ahead + out_copies + vias:
        copy.wait_send()
    slots2 = jnp.concatenate([slots_v[...], slots_v[...]], axis=1)
    index = lax.broadcasted_iota(jnp.int32, (leaves, 2 * g_total), 0)
    pick = jnp.where(index == slots2, 1.0, 0.0).astype(BF16)
    for copy in returns:
        copy.wait_recv()
    for c in range(3):
        total = returned[0, c]
        for k in range(1, 6):
            total = total + returned[k, c]
        out_ref[c, 0] = acc[c] + dot(pick, two(total))
    for copy in returns:
        copy.wait_send()


def local(shape, positions, masses, occupancy, export_slots, export_count, pair_list, pair_count):
    leaves, width = masses.shape[1:]
    g_total = export_slots.shape[1]
    pair_slots = pair_list.shape[2]
    far = pl.BlockSpec(memory_space=pltpu.HBM)
    return pl.pallas_call(
        functools.partial(kernel, shape),
        out_shape=pltpu.VMEM(positions.shape, F32),
        in_specs=[far] * 7,
        out_specs=pl.BlockSpec(memory_space=pltpu.VMEM),
        scratch_shapes=[
            pltpu.VMEM((3, leaves, width), F32),
            pltpu.VMEM((leaves, width), F32),
            pltpu.SMEM((1, leaves), jnp.int32),
            pltpu.SMEM((1, g_total), jnp.int32),
            pltpu.SMEM((1, 1), jnp.int32),
            pltpu.SMEM((2, 1, pair_slots), jnp.int32),
            pltpu.SMEM((1, 1), jnp.int32),
            pltpu.VMEM((1, g_total), jnp.int32),
            pltpu.VMEM((2, 1, pair_slots), jnp.int32),
            pltpu.VMEM((g_total, 4, width), F32),
            pltpu.VMEM((leaves + 8 * g_total, 4, width), F32),
            pltpu.VMEM((leaves, 32, width), BF16),
            pltpu.VMEM((leaves, 16, width), BF16),
            pltpu.VMEM((UNROLL, width, width), F32),
            pltpu.VMEM((UNROLL, width, width), F32),
            pltpu.VMEM((2, UNROLL, width, width), BF16),
            pltpu.VMEM((2, UNROLL, width, width), BF16),
            pltpu.VMEM((4 * leaves, width), F32),
            pltpu.VMEM((8 * pair_slots, width), F32),
            pltpu.VMEM((8, 3, g_total, width), F32),
            pltpu.VMEM((2, 3, g_total, width), F32),
            pltpu.VMEM((2, 3, g_total, width), F32),
            pltpu.VMEM((6, 3, g_total, width), F32),
            pltpu.VMEM((3, leaves, width), F32),
            pltpu.SemaphoreType.DMA((9,)),
            pltpu.SemaphoreType.DMA((8,)),
            pltpu.SemaphoreType.DMA((8,)),
            pltpu.SemaphoreType.DMA((8,)),
            pltpu.SemaphoreType.DMA((8,)),
        ],
        compiler_params=pltpu.CompilerParams(collective_id=0, has_side_effects=True),
    )(positions, masses, occupancy, export_slots, export_count, pair_list, pair_count)


def solution(mesh):
    return jax.shard_map(
        functools.partial(local, (mesh.shape["space"], mesh.shape["sub"])),
        mesh=mesh,
        in_specs=(
            P(None, "space", "sub", None),
            P("space", "sub", None),
            P("space", "sub"),
            P("space", "sub"),
            P("space", "sub"),
            P(None, "space", "sub"),
            P("space", "sub"),
        ),
        out_specs=P(None, "space", "sub", None),
        check_vma=False,
    )
```

```python
import functools

import jax
import jax.numpy as jnp
from jax import lax
from jax.experimental import pallas as pl
from jax.experimental.pallas import tpu as pltpu
from jax.sharding import PartitionSpec as P

OFFSETS = ((-1, -1), (-1, 0), (-1, 1), (0, -1), (0, 1), (1, -1), (1, 0), (1, 1))
SOFTEN = 0.05
CENTRE = 0.75
MESH = pl.DeviceIdType.MESH
F32 = jnp.float32
BF16 = jnp.bfloat16
UNROLL = 8


def split3(x):
    h = x.astype(BF16).astype(F32)
    rest = x - h
    m = rest.astype(BF16).astype(F32)
    return h, m, rest - m


def masks():
    row = lax.broadcasted_iota(jnp.int32, (8, 128), 0)
    return row < 4, (row == 3) | (row == 7)


def two_leaves(first, second, low, last):
    both = jnp.concatenate([first, second], axis=0)
    mass = jnp.where(low, both[3:4, :], both[7:8, :])
    return jnp.where(last, 0.0, both - CENTRE), mass


def swap(x):
    return pltpu.roll(x, 4, 0)


def squared(centred, last, extra):
    t = centred * centred
    t = t + pltpu.roll(t, 1, 0)
    t = t + pltpu.roll(t, 2, 0) + extra
    return split3(jnp.where(last, t, centred))


def halves(low, upper, lower):
    return jnp.where(low, upper, swap(lower)), jnp.where(low, swap(upper), lower)


def stacked(low, blocks):
    parts = [halves(low, upper, lower) for upper, lower in blocks]
    zero = jnp.zeros((8, 128), F32)
    pad = [zero] * (4 - len(parts)) if len(parts) > 2 else []
    return [jnp.concatenate([p[i] for p in parts] + pad, axis=0).astype(BF16) for i in range(2)]


def target_features(centred, low, last):
    h, m, l = squared(centred, last, 0.0)
    h1 = jnp.where(last, 1.0, h)
    m1 = jnp.where(last, 1.0, m)
    return stacked(low, [(h, m), (l, h1), (h1, m1)])


def source_features(centred, low, last):
    h, m, l = squared(centred, last, SOFTEN)
    head = jnp.where(last, 1.0, -2.0 * h)
    minus = -2.0 * m
    return stacked(
        low,
        [
            (head, head),
            (head, jnp.where(last, h, minus)),
            (jnp.where(last, m, -2.0 * l), jnp.where(last, l, minus)),
        ],
    )


def moments(centred, mass, low, last):
    h, m, l = split3(jnp.where(last, 1.0, centred) * mass)
    return stacked(low, [(h, m), (l, jnp.zeros_like(l))])


def weights(softened):
    falloff = jnp.maximum((1.0 + SOFTEN) - softened, 0.0)
    root = lax.rsqrt(softened)
    scaled = falloff * root
    return scaled * scaled * root


def force(first, second, centred, mass, low):
    a, b = (t[0:8, 0:128] + t[0:8, 128:256] + (t[8:16, 0:128] + t[8:16, 128:256]) for t in (first, second))
    both = jnp.where(low, a, b) + swap(jnp.where(low, b, a))
    return mass * (both - centred * jnp.where(low, both[3:4, :], both[7:8, :]))


def dot(a, b):
    return jnp.dot(a, b, preferred_element_type=F32)


def distances(targets, sources):
    zero = jnp.zeros_like(sources[0])
    source = jnp.concatenate(
        [
            jnp.concatenate([sources[0], zero], axis=1),
            jnp.concatenate([zero, sources[1]], axis=1),
        ],
        axis=0,
    )
    return dot(jnp.concatenate(targets, axis=0).T, source)


def weigh(dist, buf):
    for j in range(UNROLL):
        w = weights(dist[j])
        buf[0, j] = w.astype(BF16)
        buf[1, j] = (w - buf[0, j].astype(F32)).astype(BF16)


def beside(buf, j):
    return jnp.concatenate([buf[0, j], buf[1, j]], axis=1)


def turned(buf, j):
    return jnp.concatenate([buf[0, j].T, buf[1, j].T], axis=1)


def pipeline(groups, measure, combine, dists, bufs):
    measure(0, dists[0])
    weigh(dists[0], bufs[0])
    measure(1, dists[1])

    def step(i, carry):
        combine(2 * i, bufs[0])
        weigh(dists[1], bufs[1])
        measure(2 * i + 2, dists[0])
        combine(2 * i + 1, bufs[1])
        weigh(dists[0], bufs[0])
        measure(2 * i + 3, dists[1])
        return carry

    lax.fori_loop(0, groups // 2 - 1, step, 0)
    combine(groups - 2, bufs[0])
    weigh(dists[1], bufs[1])
    combine(groups - 1, bufs[1])


def slot_of(a, b):
    if a == 0:
        return 3 + (b + 1) // 2
    return b + 1 if a < 0 else b + 6


def kernel(
    shape,
    pos_hbm, mass_hbm, occ_hbm, slots_hbm, ecount_hbm, pairs_hbm, pcount_hbm,
    out_ref,
    pos_v, mass_v, occ_s, slots_s, ecount_s, pairs_s, pcount_s, slots_v, pairs_v,
    sent, pool, target_o, moment_o, dist0, dist1, buf0, buf1, self_f, pair_f, ghost_f, via, passed, returned, acc, back_f, pick_v, pick_s,
    in_sem, send_sem, recv_sem, send2_sem, recv2_sem,
):
    n_space, n_sub = shape
    leaves = pos_v.shape[1]
    g_total = sent.shape[0]
    pair_slots = pairs_v.shape[2]
    s = lax.axis_index("space")
    r = lax.axis_index("sub")
    inner = 1 - 2 * lax.rem(r, 2)
    outer = -inner

    def place(a, b):
        return (lax.rem(s + a + n_space, n_space), lax.rem(r + b + n_sub, n_sub))

    loads = [
        pltpu.make_async_copy(src, dst, in_sem.at[i])
        for i, (src, dst) in enumerate(
            [
                (slots_hbm, slots_s),
                (occ_hbm, occ_s),
                (ecount_hbm, ecount_s),
                (pcount_hbm, pcount_s),
                (pos_hbm.at[:, 0], pos_v),
                (mass_hbm.at[0], mass_v),
                (pairs_hbm, pairs_s),
                (slots_hbm, slots_v),
                (pairs_hbm, pairs_v),
            ]
        )
    ]
    for load in loads:
        load.start()
    barrier = pltpu.get_barrier_semaphore()
    for a, b in OFFSETS:
        pl.semaphore_signal(barrier, inc=1, device_id=place(a, b), device_id_type=MESH)
    for load in loads:
        load.wait()

    lane = lax.broadcasted_iota(jnp.int32, (1, 128), 1)
    exported = ecount_s[0, 0]

    def gather(i, carry):
        for j in range(8):
            g = i * 8 + j
            slot = slots_s[0, g]
            for c in range(3):
                sent[g, pl.ds(c, 1), :] = pos_v[c, pl.ds(slot, 1), :]
            live = jnp.where(g < exported, occ_s[0, slot], 0)
            sent[g, pl.ds(3, 1), :] = jnp.where(lane < live, mass_v[pl.ds(slot, 1), :], 0.0)
        return carry

    lax.fori_loop(0, g_total // 8, gather, 0)
    pl.semaphore_wait(barrier, len(OFFSETS))

    def remote(src, dst, send, recv, role, a, b):
        copy = pltpu.make_async_remote_copy(
            src_ref=src,
            dst_ref=dst,
            send_sem=send.at[role],
            recv_sem=recv.at[role],
            device_id=place(a, b),
            device_id_type=MESH,
        )
        copy.start()
        return copy

    def ghosts_at(slot):
        return pool.at[pl.ds(leaves + slot * g_total, g_total)]

    def export(role, a, b, slot, src=sent):
        return remote(src, ghosts_at(slot), send_sem, recv_sem, role, a, b)

    ahead = [export(0, 1, 0, slot_of(-1, 0)), export(1, -1, 0, slot_of(1, 0))]
    out_copies = [
        export(4, 1, outer, inner + 1),
        export(5, -1, outer, inner + 6),
        export(3, 0, outer, 3 + (inner + 1) // 2),
        export(2, 0, inner, 3 + (outer + 1) // 2),
    ]

    def own(i, carry):
        for j in range(8):
            leaf = i * 8 + j
            for c in range(3):
                pool[leaf, pl.ds(c, 1), :] = pos_v[c, pl.ds(leaf, 1), :]
            pool[leaf, pl.ds(3, 1), :] = jnp.where(
                lane < occ_s[0, leaf], mass_v[pl.ds(leaf, 1), :], 0.0
            )
        return carry

    lax.fori_loop(0, leaves // 8, own, 0)

    def rows_at(i):
        return pl.ds(pl.multiple_of(8 * i, 8), 8)

    def self_measure(group, dist):
        low, last = masks()
        for j in range(0, UNROLL, 2):
            leaf = group * UNROLL + j
            centred, mass = two_leaves(pool[leaf], pool[leaf + 1], low, last)
            targets = target_features(centred, low, last)
            both = distances(targets, source_features(centred, low, last))
            mom = moments(centred, mass, low, last)
            for i in range(2):
                dist[j + i] = both[:, i * 128 : (i + 1) * 128]
                target_o[leaf + i] = targets[i]
                moment_o[leaf + i] = mom[i]

    def self_combine(group, buf):
        low, last = masks()
        for j in range(0, UNROLL, 2):
            leaf = group * UNROLL + j
            centred, mass = two_leaves(pool[leaf], pool[leaf + 1], low, last)
            sums = [dot(moment_o[leaf + i], beside(buf, j + i)) for i in range(2)]
            self_f[rows_at(group * (UNROLL // 2) + j // 2), :] = force(*sums, centred, mass, low)

    stages = ((dist0, dist1), (buf0, buf1))
    pipeline(leaves // UNROLL, self_measure, self_combine, *stages)

    for role, copy in enumerate(ahead):
        copy.wait_recv()
        a = 2 * role - 1
        slot = slot_of(a, 0)
        out_copies.append(export(6 + role, 0, inner, (outer + 1) if a < 0 else (outer + 6), ghosts_at(slot)))
    key = jnp.concatenate([pairs_v[0], pairs_v[1]], axis=1)
    slot = lax.broadcasted_iota(jnp.int32, (1, 2 * pair_slots), 1)
    slot = jnp.where(slot < pair_slots, slot, slot - pair_slots)
    key = jnp.where(slot < pcount_s[0, 0], key, -1)
    key = jnp.concatenate([key, key], axis=1)

    order = [inner + 1, inner + 6, 3 + (inner + 1) // 2]
    order += [outer + 1, outer + 6, 3 + (outer + 1) // 2, slot_of(-1, 0), slot_of(1, 0)]
    index = lax.broadcasted_iota(jnp.int32, (g_total, 4 * pair_slots), 0)
    for k, slot in enumerate(order):
        pick = jnp.where(index + (leaves + slot * g_total) == key, 1.0, 0.0)
        pick_v[k * g_total : (k + 1) * g_total, :] = pick.astype(BF16)
    index = lax.broadcasted_iota(jnp.int32, (leaves, 4 * pair_slots), 0)
    pick_v[8 * g_total :, :] = jnp.where(index == key, 1.0, 0.0).astype(BF16)
    slots2 = jnp.concatenate([slots_v[...], slots_v[...]], axis=1)
    index = lax.broadcasted_iota(jnp.int32, (leaves, 2 * g_total), 0)
    pick_s[...] = jnp.where(index == slots2, 1.0, 0.0).astype(BF16)

    for copy in out_copies:
        copy.wait_recv()

    def pair_measure(group, dist):
        low, last = masks()
        for j in range(0, UNROLL, 2):
            p = group * UNROLL + j
            centred, mass = two_leaves(pool[pairs_s[1, 0, p]], pool[pairs_s[1, 0, p + 1]], low, last)
            targets = [target_o[pairs_s[0, 0, p]], target_o[pairs_s[0, 0, p + 1]]]
            both = distances(targets, source_features(centred, low, last))
            for i in range(2):
                dist[j + i] = both[:, i * 128 : (i + 1) * 128]

    def pair_combine(group, buf):
        low, last = masks()
        for j in range(0, UNROLL, 2):
            p = group * UNROLL + j
            at = group * (UNROLL // 2) + j // 2
            targets = [pairs_s[0, 0, p], pairs_s[0, 0, p + 1]]
            t_centred, t_mass = two_leaves(*[pool[t] for t in targets], low, last)
            centred, mass = two_leaves(pool[pairs_s[1, 0, p]], pool[pairs_s[1, 0, p + 1]], low, last)
            mom = moments(centred, mass, low, last)
            sums = [dot(moment_o[targets[i]], beside(buf, j + i)) for i in range(2)]
            pair_f[rows_at(pair_slots // 2 + at), :] = force(*sums, centred, mass, low)
            sums = [dot(mom[i], turned(buf, j + i)) for i in range(2)]
            pair_f[rows_at(at), :] = force(*sums, t_centred, t_mass, low)

    pipeline(pair_slots // UNROLL, pair_measure, pair_combine, *stages)

    def two(x):
        h = x.astype(BF16)
        return jnp.concatenate([h, (x - h.astype(F32)).astype(BF16)], axis=0)

    results = two(
        jnp.concatenate([pair_f[pl.ds(c, 2 * pair_slots, stride=4), :] for c in range(3)], axis=1)
    )

    ghosts = dot(pick_v[0 : 8 * g_total, :], results)
    for k in range(8):
        for c in range(3):
            ghost_f[k, c] = ghosts[k * g_total : (k + 1) * g_total, c * 128 : (c + 1) * 128]

    def back(role, a, b, src, dst):
        return pltpu.make_async_remote_copy(
            src_ref=src,
            dst_ref=dst,
            send_sem=send2_sem.at[role],
            recv_sem=recv2_sem.at[role],
            device_id=place(a, b),
            device_id_type=MESH,
        )

    vias = [back(i, 0, inner, ghost_f.at[i], via.at[i]) for i in range(2)]
    across = [back(i, 2 * i - 1, inner, ghost_f.at[i], returned.at[6 + i]) for i in range(2)]
    straight = [back(6 + i, 2 * i - 1, 0, ghost_f.at[6 + i], returned.at[4 + i]) for i in range(2)]
    summed = [back(6 + i, 2 * i - 1, 0, passed.at[i], returned.at[4 + i]) for i in range(2)]
    returns = [
        back(3, -1, outer, ghost_f.at[3], returned.at[1]),
        back(4, 1, outer, ghost_f.at[4], returned.at[2]),
        back(5, 0, outer, ghost_f.at[5], returned.at[3]),
        back(2, 0, inner, ghost_f.at[2], returned.at[0]),
    ]
    second_core = inner < 0

    @pl.when(second_core)
    def _():
        for copy in vias + returns + straight:
            copy.start()

    @pl.when(jnp.logical_not(second_core))
    def _():
        for copy in across + returns:
            copy.start()
        for i, copy in enumerate(vias):
            copy.wait_recv()
            passed[i] = ghost_f[6 + i] + via[i]
            summed[i].start()

    mine = dot(pick_v[8 * g_total :, :], results)
    for c in range(3):
        acc[c] = mine[:, c * 128 : (c + 1) * 128] + self_f[pl.ds(c, leaves, stride=4), :]
    for copy in ahead + out_copies + vias:
        copy.wait_send()
    for copy in returns + straight:
        copy.wait_recv()
    for c in range(3):
        total = returned[0, c]
        for k in range(1, 6):
            total = total + returned[k, c]
        back_f[c] = total

    @pl.when(second_core)
    def _():
        for copy in across:
            copy.wait_recv()
        for c in range(3):
            back_f[c] = back_f[c] + (returned[6, c] + returned[7, c])

    for c in range(3):
        out_ref[c, 0] = acc[c] + dot(pick_s[...], two(back_f[c]))
    for copy in returns + straight:
        copy.wait_send()


def local(shape, positions, masses, occupancy, export_slots, export_count, pair_list, pair_count):
    leaves, width = masses.shape[1:]
    g_total = export_slots.shape[1]
    pair_slots = pair_list.shape[2]
    far = pl.BlockSpec(memory_space=pltpu.HBM)
    return pl.pallas_call(
        functools.partial(kernel, shape),
        out_shape=pltpu.VMEM(positions.shape, F32),
        in_specs=[far] * 7,
        out_specs=pl.BlockSpec(memory_space=pltpu.VMEM),
        scratch_shapes=[
            pltpu.VMEM((3, leaves, width), F32),
            pltpu.VMEM((leaves, width), F32),
            pltpu.SMEM((1, leaves), jnp.int32),
            pltpu.SMEM((1, g_total), jnp.int32),
            pltpu.SMEM((1, 1), jnp.int32),
            pltpu.SMEM((2, 1, pair_slots), jnp.int32),
            pltpu.SMEM((1, 1), jnp.int32),
            pltpu.VMEM((1, g_total), jnp.int32),
            pltpu.VMEM((2, 1, pair_slots), jnp.int32),
            pltpu.VMEM((g_total, 4, width), F32),
            pltpu.VMEM((leaves + 8 * g_total, 4, width), F32),
            pltpu.VMEM((leaves, 32, width), BF16),
            pltpu.VMEM((leaves, 16, width), BF16),
            pltpu.VMEM((UNROLL, width, width), F32),
            pltpu.VMEM((UNROLL, width, width), F32),
            pltpu.VMEM((2, UNROLL, width, width), BF16),
            pltpu.VMEM((2, UNROLL, width, width), BF16),
            pltpu.VMEM((4 * leaves, width), F32),
            pltpu.VMEM((8 * pair_slots, width), F32),
            pltpu.VMEM((8, 3, g_total, width), F32),
            pltpu.VMEM((2, 3, g_total, width), F32),
            pltpu.VMEM((2, 3, g_total, width), F32),
            pltpu.VMEM((8, 3, g_total, width), F32),
            pltpu.VMEM((3, leaves, width), F32),
            pltpu.VMEM((3, g_total, width), F32),
            pltpu.VMEM((8 * g_total + leaves, 4 * pair_slots), BF16),
            pltpu.VMEM((leaves, 2 * g_total), BF16),
            pltpu.SemaphoreType.DMA((9,)),
            pltpu.SemaphoreType.DMA((8,)),
            pltpu.SemaphoreType.DMA((8,)),
            pltpu.SemaphoreType.DMA((8,)),
            pltpu.SemaphoreType.DMA((8,)),
        ],
        compiler_params=pltpu.CompilerParams(collective_id=0, has_side_effects=True),
    )(positions, masses, occupancy, export_slots, export_count, pair_list, pair_count)


def solution(mesh):
    return jax.shard_map(
        functools.partial(local, (mesh.shape["space"], mesh.shape["sub"])),
        mesh=mesh,
        in_specs=(
            P(None, "space", "sub", None),
            P("space", "sub", None),
            P("space", "sub"),
            P("space", "sub"),
            P("space", "sub"),
            P(None, "space", "sub"),
            P("space", "sub"),
        ),
        out_specs=P(None, "space", "sub", None),
        check_vma=False,
    )
```

```python
import functools

import jax
import jax.numpy as jnp
from jax import lax
from jax.experimental import pallas as pl
from jax.experimental.pallas import tpu as pltpu
from jax.sharding import PartitionSpec as P

OFFSETS = ((-1, -1), (-1, 0), (-1, 1), (0, -1), (0, 1), (1, -1), (1, 0), (1, 1))
SOFTEN = 0.05
CENTRE = 0.75
MESH = pl.DeviceIdType.MESH
F32 = jnp.float32
BF16 = jnp.bfloat16
UNROLL = 8


def split3(x):
    h = x.astype(BF16).astype(F32)
    rest = x - h
    m = rest.astype(BF16).astype(F32)
    return h, m, rest - m


def masks():
    row = lax.broadcasted_iota(jnp.int32, (8, 128), 0)
    return row < 4, (row == 3) | (row == 7)


def two_leaves(first, second, low, last):
    both = jnp.concatenate([first, second], axis=0)
    mass = jnp.where(low, both[3:4, :], both[7:8, :])
    return jnp.where(last, 0.0, both - CENTRE), mass


def swap(x):
    return pltpu.roll(x, 4, 0)


def squared(centred, last, extra):
    t = centred * centred
    t = t + pltpu.roll(t, 1, 0)
    t = t + pltpu.roll(t, 2, 0) + extra
    return split3(jnp.where(last, t, centred))


def halves(low, upper, lower):
    return jnp.where(low, upper, swap(lower)), jnp.where(low, swap(upper), lower)


def stacked(low, blocks):
    parts = [halves(low, upper, lower) for upper, lower in blocks]
    zero = jnp.zeros((8, 128), F32)
    pad = [zero] * (4 - len(parts)) if len(parts) > 2 else []
    return [jnp.concatenate([p[i] for p in parts] + pad, axis=0).astype(BF16) for i in range(2)]


def target_features(centred, low, last):
    h, m, l = squared(centred, last, 0.0)
    h1 = jnp.where(last, 1.0, h)
    m1 = jnp.where(last, 1.0, m)
    return stacked(low, [(h, m), (l, h1), (h1, m1)])


def source_features(centred, low, last):
    h, m, l = squared(centred, last, SOFTEN)
    head = jnp.where(last, 1.0, -2.0 * h)
    minus = -2.0 * m
    return stacked(
        low,
        [
            (head, head),
            (head, jnp.where(last, h, minus)),
            (jnp.where(last, m, -2.0 * l), jnp.where(last, l, minus)),
        ],
    )


def moments(centred, mass, low, last):
    h, m, l = split3(jnp.where(last, 1.0, centred) * mass)
    return stacked(low, [(h, m), (l, jnp.zeros_like(l))])


def weights(softened):
    falloff = jnp.maximum((1.0 + SOFTEN) - softened, 0.0)
    root = lax.rsqrt(softened)
    scaled = falloff * root
    return scaled * scaled * root


def force(first, second, centred, mass, low):
    a, b = (t[0:8, 0:128] + t[0:8, 128:256] + (t[8:16, 0:128] + t[8:16, 128:256]) for t in (first, second))
    both = jnp.where(low, a, b) + swap(jnp.where(low, b, a))
    return mass * (both - centred * jnp.where(low, both[3:4, :], both[7:8, :]))


def dot(a, b):
    return jnp.dot(a, b, preferred_element_type=F32)


def distances(targets, sources):
    zero = jnp.zeros_like(sources[0])
    source = jnp.concatenate(
        [
            jnp.concatenate([sources[0], zero], axis=1),
            jnp.concatenate([zero, sources[1]], axis=1),
        ],
        axis=0,
    )
    return dot(jnp.concatenate(targets, axis=0).T, source)


def weigh(dist, buf):
    for j in range(UNROLL):
        w = weights(dist[j])
        buf[0, j] = w.astype(BF16)
        buf[1, j] = (w - buf[0, j].astype(F32)).astype(BF16)


def beside(buf, j):
    return jnp.concatenate([buf[0, j], buf[1, j]], axis=1)


def turned(buf, j):
    return jnp.concatenate([buf[0, j].T, buf[1, j].T], axis=1)


def pipeline(groups, measure, combine, dists, bufs, unroll=False):
    measure(0, dists[0])
    weigh(dists[0], bufs[0])
    measure(1, dists[1])

    def step(i, carry):
        combine(2 * i, bufs[0])
        weigh(dists[1], bufs[1])
        measure(2 * i + 2, dists[0])
        combine(2 * i + 1, bufs[1])
        weigh(dists[0], bufs[0])
        measure(2 * i + 3, dists[1])
        return carry

    if unroll:
        for i in range(groups // 2 - 1):
            step(i, 0)
    else:
        lax.fori_loop(0, groups // 2 - 1, step, 0)
    combine(groups - 2, bufs[0])
    weigh(dists[1], bufs[1])
    combine(groups - 1, bufs[1])


def slot_of(a, b):
    if a == 0:
        return 3 + (b + 1) // 2
    return b + 1 if a < 0 else b + 6


def kernel(
    shape,
    pos_hbm, mass_hbm, occ_hbm, slots_hbm, ecount_hbm, pairs_hbm, pcount_hbm,
    out_ref,
    pos_v, mass_v, occ_s, slots_s, ecount_s, pairs_s, pcount_s, slots_v, pairs_v,
    sent, pool, target_o, moment_o, dist0, dist1, buf0, buf1, self_f, pair_f, ghost_f, via, passed, returned, acc, back_f, pick_v, pick_s,
    in_sem, send_sem, recv_sem, send2_sem, recv2_sem,
):
    n_space, n_sub = shape
    leaves = pos_v.shape[1]
    g_total = sent.shape[0]
    pair_slots = pairs_v.shape[2]
    s = lax.axis_index("space")
    r = lax.axis_index("sub")
    inner = 1 - 2 * lax.rem(r, 2)
    outer = -inner

    def place(a, b):
        return (lax.rem(s + a + n_space, n_space), lax.rem(r + b + n_sub, n_sub))

    loads = [
        pltpu.make_async_copy(src, dst, in_sem.at[i])
        for i, (src, dst) in enumerate(
            [
                (slots_hbm, slots_s),
                (occ_hbm, occ_s),
                (ecount_hbm, ecount_s),
                (pcount_hbm, pcount_s),
                (pos_hbm.at[:, 0], pos_v),
                (mass_hbm.at[0], mass_v),
                (pairs_hbm, pairs_s),
                (slots_hbm, slots_v),
                (pairs_hbm, pairs_v),
            ]
        )
    ]
    for load in loads:
        load.start()
    barrier = pltpu.get_barrier_semaphore()
    for a, b in OFFSETS:
        pl.semaphore_signal(barrier, inc=1, device_id=place(a, b), device_id_type=MESH)
    for load in loads:
        load.wait()

    lane = lax.broadcasted_iota(jnp.int32, (1, 128), 1)
    exported = ecount_s[0, 0]

    def gather(i, carry):
        for j in range(8):
            g = i * 8 + j
            slot = slots_s[0, g]
            for c in range(3):
                sent[g, pl.ds(c, 1), :] = pos_v[c, pl.ds(slot, 1), :]
            live = jnp.where(g < exported, occ_s[0, slot], 0)
            sent[g, pl.ds(3, 1), :] = jnp.where(lane < live, mass_v[pl.ds(slot, 1), :], 0.0)
        return carry

    lax.fori_loop(0, g_total // 8, gather, 0)
    pl.semaphore_wait(barrier, len(OFFSETS))

    def remote(src, dst, send, recv, role, a, b):
        copy = pltpu.make_async_remote_copy(
            src_ref=src,
            dst_ref=dst,
            send_sem=send.at[role],
            recv_sem=recv.at[role],
            device_id=place(a, b),
            device_id_type=MESH,
        )
        copy.start()
        return copy

    def ghosts_at(slot):
        return pool.at[pl.ds(leaves + slot * g_total, g_total)]

    def export(role, a, b, slot, src=sent):
        return remote(src, ghosts_at(slot), send_sem, recv_sem, role, a, b)

    ahead = [export(0, 1, 0, slot_of(-1, 0)), export(1, -1, 0, slot_of(1, 0))]
    out_copies = [
        export(4, 1, outer, inner + 1),
        export(5, -1, outer, inner + 6),
        export(3, 0, outer, 3 + (inner + 1) // 2),
        export(2, 0, inner, 3 + (outer + 1) // 2),
    ]

    def own(i, carry):
        for j in range(8):
            leaf = i * 8 + j
            for c in range(3):
                pool[leaf, pl.ds(c, 1), :] = pos_v[c, pl.ds(leaf, 1), :]
            pool[leaf, pl.ds(3, 1), :] = jnp.where(
                lane < occ_s[0, leaf], mass_v[pl.ds(leaf, 1), :], 0.0
            )
        return carry

    lax.fori_loop(0, leaves // 8, own, 0)

    def rows_at(i):
        return pl.ds(8 * i if isinstance(i, int) else pl.multiple_of(8 * i, 8), 8)

    def self_measure(group, dist):
        low, last = masks()
        for j in range(0, UNROLL, 2):
            leaf = group * UNROLL + j
            centred, mass = two_leaves(pool[leaf], pool[leaf + 1], low, last)
            targets = target_features(centred, low, last)
            both = distances(targets, source_features(centred, low, last))
            mom = moments(centred, mass, low, last)
            for i in range(2):
                dist[j + i] = both[:, i * 128 : (i + 1) * 128]
                target_o[leaf + i] = targets[i]
                moment_o[leaf + i] = mom[i]

    def self_combine(group, buf):
        low, last = masks()
        for j in range(0, UNROLL, 2):
            leaf = group * UNROLL + j
            centred, mass = two_leaves(pool[leaf], pool[leaf + 1], low, last)
            sums = [dot(moment_o[leaf + i], beside(buf, j + i)) for i in range(2)]
            self_f[rows_at(group * (UNROLL // 2) + j // 2), :] = force(*sums, centred, mass, low)

    stages = ((dist0, dist1), (buf0, buf1))
    pipeline(leaves // UNROLL, self_measure, self_combine, *stages)

    for role, copy in enumerate(ahead):
        copy.wait_recv()
        a = 2 * role - 1
        slot = slot_of(a, 0)
        out_copies.append(export(6 + role, 0, inner, (outer + 1) if a < 0 else (outer + 6), ghosts_at(slot)))
    key = jnp.concatenate([pairs_v[0], pairs_v[1]], axis=1)
    slot = lax.broadcasted_iota(jnp.int32, (1, 2 * pair_slots), 1)
    slot = jnp.where(slot < pair_slots, slot, slot - pair_slots)
    key = jnp.where(slot < pcount_s[0, 0], key, -1)
    key = jnp.concatenate([key, key], axis=1)

    order = [inner + 1, inner + 6, 3 + (inner + 1) // 2]
    order += [outer + 1, outer + 6, 3 + (outer + 1) // 2, slot_of(-1, 0), slot_of(1, 0)]
    index = lax.broadcasted_iota(jnp.int32, (g_total, 4 * pair_slots), 0)
    for k, slot in enumerate(order):
        pick = jnp.where(index + (leaves + slot * g_total) == key, 1.0, 0.0)
        pick_v[k * g_total : (k + 1) * g_total, :] = pick.astype(BF16)
    index = lax.broadcasted_iota(jnp.int32, (leaves, 4 * pair_slots), 0)
    pick_v[8 * g_total :, :] = jnp.where(index == key, 1.0, 0.0).astype(BF16)
    slots2 = jnp.concatenate([slots_v[...], slots_v[...]], axis=1)
    index = lax.broadcasted_iota(jnp.int32, (leaves, 2 * g_total), 0)
    pick_s[...] = jnp.where(index == slots2, 1.0, 0.0).astype(BF16)

    for copy in out_copies:
        copy.wait_recv()

    def pair_measure(group, dist):
        low, last = masks()
        for j in range(0, UNROLL, 2):
            p = group * UNROLL + j
            centred, mass = two_leaves(pool[pairs_s[1, 0, p]], pool[pairs_s[1, 0, p + 1]], low, last)
            targets = [target_o[pairs_s[0, 0, p]], target_o[pairs_s[0, 0, p + 1]]]
            both = distances(targets, source_features(centred, low, last))
            for i in range(2):
                dist[j + i] = both[:, i * 128 : (i + 1) * 128]

    def pair_combine(group, buf):
        low, last = masks()
        for j in range(0, UNROLL, 2):
            p = group * UNROLL + j
            at = group * (UNROLL // 2) + j // 2
            targets = [pairs_s[0, 0, p], pairs_s[0, 0, p + 1]]
            t_centred, t_mass = two_leaves(*[pool[t] for t in targets], low, last)
            centred, mass = two_leaves(pool[pairs_s[1, 0, p]], pool[pairs_s[1, 0, p + 1]], low, last)
            mom = moments(centred, mass, low, last)
            sums = [dot(moment_o[targets[i]], beside(buf, j + i)) for i in range(2)]
            pair_f[rows_at(pair_slots // 2 + at), :] = force(*sums, centred, mass, low)
            sums = [dot(mom[i], turned(buf, j + i)) for i in range(2)]
            pair_f[rows_at(at), :] = force(*sums, t_centred, t_mass, low)

    pipeline(pair_slots // UNROLL, pair_measure, pair_combine, *stages, unroll=True)

    def two(x):
        h = x.astype(BF16)
        return jnp.concatenate([h, (x - h.astype(F32)).astype(BF16)], axis=0)

    results = two(
        jnp.concatenate([pair_f[pl.ds(c, 2 * pair_slots, stride=4), :] for c in range(3)], axis=1)
    )

    ghosts = dot(pick_v[0 : 8 * g_total, :], results)
    for k in range(8):
        for c in range(3):
            ghost_f[k, c] = ghosts[k * g_total : (k + 1) * g_total, c * 128 : (c + 1) * 128]

    def back(role, a, b, src, dst):
        return pltpu.make_async_remote_copy(
            src_ref=src,
            dst_ref=dst,
            send_sem=send2_sem.at[role],
            recv_sem=recv2_sem.at[role],
            device_id=place(a, b),
            device_id_type=MESH,
        )

    vias = [back(i, 0, inner, ghost_f.at[i], via.at[i]) for i in range(2)]
    across = [back(i, 2 * i - 1, inner, ghost_f.at[i], returned.at[6 + i]) for i in range(2)]
    straight = [back(6 + i, 2 * i - 1, 0, ghost_f.at[6 + i], returned.at[4 + i]) for i in range(2)]
    summed = [back(6 + i, 2 * i - 1, 0, passed.at[i], returned.at[4 + i]) for i in range(2)]
    returns = [
        back(3, -1, outer, ghost_f.at[3], returned.at[1]),
        back(4, 1, outer, ghost_f.at[4], returned.at[2]),
        back(5, 0, outer, ghost_f.at[5], returned.at[3]),
        back(2, 0, inner, ghost_f.at[2], returned.at[0]),
    ]
    second_core = inner < 0

    @pl.when(second_core)
    def _():
        for copy in vias + returns + straight:
            copy.start()

    @pl.when(jnp.logical_not(second_core))
    def _():
        for copy in across + returns:
            copy.start()
        for i, copy in enumerate(vias):
            copy.wait_recv()
            passed[i] = ghost_f[6 + i] + via[i]
            summed[i].start()

    mine = dot(pick_v[8 * g_total :, :], results)
    for c in range(3):
        acc[c] = mine[:, c * 128 : (c + 1) * 128] + self_f[pl.ds(c, leaves, stride=4), :]
    for copy in ahead + out_copies + vias:
        copy.wait_send()
    for copy in returns + straight:
        copy.wait_recv()
    for c in range(3):
        total = returned[0, c]
        for k in range(1, 6):
            total = total + returned[k, c]
        back_f[c] = total

    @pl.when(second_core)
    def _():
        for copy in across:
            copy.wait_recv()
        for c in range(3):
            back_f[c] = back_f[c] + (returned[6, c] + returned[7, c])

    for c in range(3):
        out_ref[c, 0] = acc[c] + dot(pick_s[...], two(back_f[c]))
    for copy in returns + straight:
        copy.wait_send()


def local(shape, positions, masses, occupancy, export_slots, export_count, pair_list, pair_count):
    leaves, width = masses.shape[1:]
    g_total = export_slots.shape[1]
    pair_slots = pair_list.shape[2]
    far = pl.BlockSpec(memory_space=pltpu.HBM)
    return pl.pallas_call(
        functools.partial(kernel, shape),
        out_shape=pltpu.VMEM(positions.shape, F32),
        in_specs=[far] * 7,
        out_specs=pl.BlockSpec(memory_space=pltpu.VMEM),
        scratch_shapes=[
            pltpu.VMEM((3, leaves, width), F32),
            pltpu.VMEM((leaves, width), F32),
            pltpu.SMEM((1, leaves), jnp.int32),
            pltpu.SMEM((1, g_total), jnp.int32),
            pltpu.SMEM((1, 1), jnp.int32),
            pltpu.SMEM((2, 1, pair_slots), jnp.int32),
            pltpu.SMEM((1, 1), jnp.int32),
            pltpu.VMEM((1, g_total), jnp.int32),
            pltpu.VMEM((2, 1, pair_slots), jnp.int32),
            pltpu.VMEM((g_total, 4, width), F32),
            pltpu.VMEM((leaves + 8 * g_total, 4, width), F32),
            pltpu.VMEM((leaves, 32, width), BF16),
            pltpu.VMEM((leaves, 16, width), BF16),
            pltpu.VMEM((UNROLL, width, width), F32),
            pltpu.VMEM((UNROLL, width, width), F32),
            pltpu.VMEM((2, UNROLL, width, width), BF16),
            pltpu.VMEM((2, UNROLL, width, width), BF16),
            pltpu.VMEM((4 * leaves, width), F32),
            pltpu.VMEM((8 * pair_slots, width), F32),
            pltpu.VMEM((8, 3, g_total, width), F32),
            pltpu.VMEM((2, 3, g_total, width), F32),
            pltpu.VMEM((2, 3, g_total, width), F32),
            pltpu.VMEM((8, 3, g_total, width), F32),
            pltpu.VMEM((3, leaves, width), F32),
            pltpu.VMEM((3, g_total, width), F32),
            pltpu.VMEM((8 * g_total + leaves, 4 * pair_slots), BF16),
            pltpu.VMEM((leaves, 2 * g_total), BF16),
            pltpu.SemaphoreType.DMA((9,)),
            pltpu.SemaphoreType.DMA((8,)),
            pltpu.SemaphoreType.DMA((8,)),
            pltpu.SemaphoreType.DMA((8,)),
            pltpu.SemaphoreType.DMA((8,)),
        ],
        compiler_params=pltpu.CompilerParams(collective_id=0, has_side_effects=True),
    )(positions, masses, occupancy, export_slots, export_count, pair_list, pair_count)


def solution(mesh):
    return jax.shard_map(
        functools.partial(local, (mesh.shape["space"], mesh.shape["sub"])),
        mesh=mesh,
        in_specs=(
            P(None, "space", "sub", None),
            P("space", "sub", None),
            P("space", "sub"),
            P("space", "sub"),
            P("space", "sub"),
            P(None, "space", "sub"),
            P("space", "sub"),
        ),
        out_specs=P(None, "space", "sub", None),
        check_vma=False,
    )
```

```python
import functools

import jax
import jax.numpy as jnp
from jax import lax
from jax.experimental import pallas as pl
from jax.experimental.pallas import tpu as pltpu
from jax.sharding import PartitionSpec as P

OFFSETS = ((-1, -1), (-1, 0), (-1, 1), (0, -1), (0, 1), (1, -1), (1, 0), (1, 1))
SOFTEN = 0.05
CENTRE = 0.75
MESH = pl.DeviceIdType.MESH
F32 = jnp.float32
BF16 = jnp.bfloat16
UNROLL = 8


def split3(x):
    h = x.astype(BF16).astype(F32)
    rest = x - h
    m = rest.astype(BF16).astype(F32)
    return h, m, rest - m


def masks():
    row = lax.broadcasted_iota(jnp.int32, (8, 128), 0)
    return row < 4, (row == 3) | (row == 7)


def two_leaves(first, second, low, last):
    both = jnp.concatenate([first, second], axis=0)
    mass = jnp.where(low, both[3:4, :], both[7:8, :])
    return jnp.where(last, 0.0, both - CENTRE), mass


def swap(x):
    return pltpu.roll(x, 4, 0)


def squared(centred, last, extra):
    t = centred * centred
    t = t + pltpu.roll(t, 1, 0)
    t = t + pltpu.roll(t, 2, 0) + extra
    return split3(jnp.where(last, t, centred))


def halves(low, upper, lower):
    return jnp.where(low, upper, swap(lower)), jnp.where(low, swap(upper), lower)


def stacked(low, blocks):
    parts = [halves(low, upper, lower) for upper, lower in blocks]
    zero = jnp.zeros((8, 128), F32)
    pad = [zero] * (4 - len(parts)) if len(parts) > 2 else []
    return [jnp.concatenate([p[i] for p in parts] + pad, axis=0).astype(BF16) for i in range(2)]


def target_features(centred, low, last):
    h, m, l = squared(centred, last, 0.0)
    h1 = jnp.where(last, 1.0, h)
    m1 = jnp.where(last, 1.0, m)
    return stacked(low, [(h, m), (l, h1), (h1, m1)])


def source_features(centred, low, last):
    h, m, l = squared(centred, last, SOFTEN)
    head = jnp.where(last, 1.0, -2.0 * h)
    minus = -2.0 * m
    return stacked(
        low,
        [
            (head, head),
            (head, jnp.where(last, h, minus)),
            (jnp.where(last, m, -2.0 * l), jnp.where(last, l, minus)),
        ],
    )


def moments(centred, mass, low, last):
    h, m, l = split3(jnp.where(last, 1.0, centred) * mass)
    return stacked(low, [(h, m), (l, jnp.zeros_like(l))])


def weights(softened):
    falloff = jnp.maximum((1.0 + SOFTEN) - softened, 0.0)
    root = lax.rsqrt(softened)
    scaled = falloff * root
    return scaled * scaled * root


def force(first, second, centred, mass, low):
    a, b = (t[0:8, 0:128] + t[0:8, 128:256] + (t[8:16, 0:128] + t[8:16, 128:256]) for t in (first, second))
    both = jnp.where(low, a, b) + swap(jnp.where(low, b, a))
    return mass * (both - centred * jnp.where(low, both[3:4, :], both[7:8, :]))


def dot(a, b):
    return jnp.dot(a, b, preferred_element_type=F32)


def distances(targets, sources):
    zero = jnp.zeros_like(sources[0])
    source = jnp.concatenate(
        [
            jnp.concatenate([sources[0], zero], axis=1),
            jnp.concatenate([zero, sources[1]], axis=1),
        ],
        axis=0,
    )
    return dot(jnp.concatenate(targets, axis=0).T, source)


def weigh(dist, buf):
    for j in range(UNROLL):
        w = weights(dist[j])
        buf[0, j] = w.astype(BF16)
        buf[1, j] = (w - buf[0, j].astype(F32)).astype(BF16)


def beside(buf, j):
    return jnp.concatenate([buf[0, j], buf[1, j]], axis=1)


def turned(buf, j):
    return jnp.concatenate([buf[0, j].T, buf[1, j].T], axis=1)


def pipeline(groups, measure, combine, dists, bufs, unroll=False):
    measure(0, dists[0])
    weigh(dists[0], bufs[0])
    measure(1, dists[1])

    def step(i, carry):
        combine(2 * i, bufs[0])
        weigh(dists[1], bufs[1])
        measure(2 * i + 2, dists[0])
        combine(2 * i + 1, bufs[1])
        weigh(dists[0], bufs[0])
        measure(2 * i + 3, dists[1])
        return carry

    if unroll:
        for i in range(groups // 2 - 1):
            step(i, 0)
    else:
        lax.fori_loop(0, groups // 2 - 1, step, 0)
    combine(groups - 2, bufs[0])
    weigh(dists[1], bufs[1])
    combine(groups - 1, bufs[1])


def slot_of(a, b):
    if a == 0:
        return 3 + (b + 1) // 2
    return b + 1 if a < 0 else b + 6


def kernel(
    shape,
    pos_hbm, mass_hbm, occ_hbm, slots_hbm, ecount_hbm, pairs_hbm, pcount_hbm,
    out_ref,
    pos_v, mass_v, occ_s, slots_s, ecount_s, pairs_s, pcount_s, slots_v, pairs_v,
    sent, pool, target_o, moment_o, dist0, dist1, buf0, buf1, self_f, pair_f, ghost_f, via, passed, returned, acc, back_f, pick_v, pick_s,
    in_sem, send_sem, recv_sem, send2_sem, recv2_sem,
):
    n_space, n_sub = shape
    leaves = pos_v.shape[1]
    g_total = sent.shape[0]
    pair_slots = pairs_v.shape[2]
    s = lax.axis_index("space")
    r = lax.axis_index("sub")
    inner = 1 - 2 * lax.rem(r, 2)
    outer = -inner

    def place(a, b):
        return (lax.rem(s + a + n_space, n_space), lax.rem(r + b + n_sub, n_sub))

    loads = [
        pltpu.make_async_copy(src, dst, in_sem.at[i])
        for i, (src, dst) in enumerate(
            [
                (slots_hbm, slots_s),
                (occ_hbm, occ_s),
                (ecount_hbm, ecount_s),
                (pcount_hbm, pcount_s),
                (pos_hbm.at[:, 0], pos_v),
                (mass_hbm.at[0], mass_v),
                (pairs_hbm, pairs_s),
                (slots_hbm, slots_v),
                (pairs_hbm, pairs_v),
            ]
        )
    ]
    for load in loads:
        load.start()
    barrier = pltpu.get_barrier_semaphore()
    for a, b in OFFSETS:
        pl.semaphore_signal(barrier, inc=1, device_id=place(a, b), device_id_type=MESH)
    for load in loads:
        load.wait()

    lane = lax.broadcasted_iota(jnp.int32, (1, 128), 1)
    exported = ecount_s[0, 0]

    def gather(i, carry):
        for j in range(8):
            g = i * 8 + j
            slot = slots_s[0, g]
            for c in range(3):
                sent[g, pl.ds(c, 1), :] = pos_v[c, pl.ds(slot, 1), :]
            live = jnp.where(g < exported, occ_s[0, slot], 0)
            sent[g, pl.ds(3, 1), :] = jnp.where(lane < live, mass_v[pl.ds(slot, 1), :], 0.0)
        return carry

    lax.fori_loop(0, g_total // 8, gather, 0)
    pl.semaphore_wait(barrier, len(OFFSETS))

    def remote(src, dst, send, recv, role, a, b):
        copy = pltpu.make_async_remote_copy(
            src_ref=src,
            dst_ref=dst,
            send_sem=send.at[role],
            recv_sem=recv.at[role],
            device_id=place(a, b),
            device_id_type=MESH,
        )
        copy.start()
        return copy

    def ghosts_at(slot):
        return pool.at[pl.ds(leaves + slot * g_total, g_total)]

    def export(role, a, b, slot, src=sent):
        return remote(src, ghosts_at(slot), send_sem, recv_sem, role, a, b)

    ahead = [export(0, 1, 0, slot_of(-1, 0)), export(1, -1, 0, slot_of(1, 0))]
    out_copies = [
        export(4, 1, outer, inner + 1),
        export(5, -1, outer, inner + 6),
        export(3, 0, outer, 3 + (inner + 1) // 2),
        export(2, 0, inner, 3 + (outer + 1) // 2),
    ]

    def own(i, carry):
        for j in range(8):
            leaf = i * 8 + j
            for c in range(3):
                pool[leaf, pl.ds(c, 1), :] = pos_v[c, pl.ds(leaf, 1), :]
            pool[leaf, pl.ds(3, 1), :] = jnp.where(
                lane < occ_s[0, leaf], mass_v[pl.ds(leaf, 1), :], 0.0
            )
        return carry

    lax.fori_loop(0, leaves // 8, own, 0)

    def rows_at(i):
        return pl.ds(8 * i if isinstance(i, int) else pl.multiple_of(8 * i, 8), 8)

    def self_measure(group, dist):
        low, last = masks()
        for j in range(0, UNROLL, 2):
            leaf = group * UNROLL + j
            centred, mass = two_leaves(pool[leaf], pool[leaf + 1], low, last)
            targets = target_features(centred, low, last)
            both = distances(targets, source_features(centred, low, last))
            mom = moments(centred, mass, low, last)
            for i in range(2):
                dist[j + i] = both[:, i * 128 : (i + 1) * 128]
                target_o[leaf + i] = targets[i]
                moment_o[leaf + i] = mom[i]

    def self_combine(group, buf):
        low, last = masks()
        for j in range(0, UNROLL, 2):
            leaf = group * UNROLL + j
            centred, mass = two_leaves(pool[leaf], pool[leaf + 1], low, last)
            sums = [dot(moment_o[leaf + i], beside(buf, j + i)) for i in range(2)]
            self_f[rows_at(group * (UNROLL // 2) + j // 2), :] = force(*sums, centred, mass, low)

    stages = ((dist0, dist1), (buf0, buf1))
    pipeline(leaves // UNROLL, self_measure, self_combine, *stages)

    for role, copy in enumerate(ahead):
        copy.wait_recv()
        a = 2 * role - 1
        slot = slot_of(a, 0)
        out_copies.append(export(6 + role, 0, inner, (outer + 1) if a < 0 else (outer + 6), ghosts_at(slot)))
    key = jnp.concatenate([pairs_v[0], pairs_v[1]], axis=1)
    slot = lax.broadcasted_iota(jnp.int32, (1, 2 * pair_slots), 1)
    slot = jnp.where(slot < pair_slots, slot, slot - pair_slots)
    key = jnp.where(slot < pcount_s[0, 0], key, -1)
    key = jnp.concatenate([key, key], axis=1)

    order = [inner + 1, inner + 6, 3 + (inner + 1) // 2]
    order += [outer + 1, outer + 6, 3 + (outer + 1) // 2, slot_of(-1, 0), slot_of(1, 0)]
    index = lax.broadcasted_iota(jnp.int32, (g_total, 4 * pair_slots), 0)
    for k, slot in enumerate(order):
        pick = jnp.where(index + (leaves + slot * g_total) == key, 1.0, 0.0)
        pick_v[k * g_total : (k + 1) * g_total, :] = pick.astype(BF16)
    index = lax.broadcasted_iota(jnp.int32, (leaves, 4 * pair_slots), 0)
    pick_v[8 * g_total :, :] = jnp.where(index == key, 1.0, 0.0).astype(BF16)
    slots2 = jnp.concatenate([slots_v[...], slots_v[...]], axis=1)
    index = lax.broadcasted_iota(jnp.int32, (leaves, 2 * g_total), 0)
    pick_s[...] = jnp.where(index == slots2, 1.0, 0.0).astype(BF16)

    for copy in out_copies:
        copy.wait_recv()

    def pair_measure(group, dist):
        low, last = masks()
        for j in range(0, UNROLL, 2):
            p = group * UNROLL + j
            centred, mass = two_leaves(pool[pairs_s[1, 0, p]], pool[pairs_s[1, 0, p + 1]], low, last)
            targets = [target_o[pairs_s[0, 0, p]], target_o[pairs_s[0, 0, p + 1]]]
            both = distances(targets, source_features(centred, low, last))
            for i in range(2):
                dist[j + i] = both[:, i * 128 : (i + 1) * 128]

    def pair_combine(group, buf):
        low, last = masks()
        for j in range(0, UNROLL, 2):
            p = group * UNROLL + j
            at = group * (UNROLL // 2) + j // 2
            targets = [pairs_s[0, 0, p], pairs_s[0, 0, p + 1]]
            t_centred, t_mass = two_leaves(*[pool[t] for t in targets], low, last)
            centred, mass = two_leaves(pool[pairs_s[1, 0, p]], pool[pairs_s[1, 0, p + 1]], low, last)
            mom = moments(centred, mass, low, last)
            sums = [dot(moment_o[targets[i]], beside(buf, j + i)) for i in range(2)]
            pair_f[rows_at(pair_slots // 2 + at), :] = force(*sums, centred, mass, low)
            sums = [dot(mom[i], turned(buf, j + i)) for i in range(2)]
            pair_f[rows_at(at), :] = force(*sums, t_centred, t_mass, low)

    pipeline(pair_slots // UNROLL, pair_measure, pair_combine, *stages, unroll=True)

    def two(x):
        h = x.astype(BF16)
        return jnp.concatenate([h, (x - h.astype(F32)).astype(BF16)], axis=0)

    results = two(
        jnp.concatenate([pair_f[pl.ds(c, 2 * pair_slots, stride=4), :] for c in range(3)], axis=1)
    )

    ghosts = dot(pick_v[0 : 8 * g_total, :], results)
    for k in range(8):
        for c in range(3):
            ghost_f[k, c] = ghosts[k * g_total : (k + 1) * g_total, c * 128 : (c + 1) * 128]

    def back(role, a, b, src, dst):
        return pltpu.make_async_remote_copy(
            src_ref=src,
            dst_ref=dst,
            send_sem=send2_sem.at[role],
            recv_sem=recv2_sem.at[role],
            device_id=place(a, b),
            device_id_type=MESH,
        )

    vias = [back(i, 0, inner, ghost_f.at[i], via.at[i]) for i in range(2)]
    across = [back(i, 2 * i - 1, inner, ghost_f.at[i], returned.at[6 + i]) for i in range(2)]
    straight = [back(6 + i, 2 * i - 1, 0, ghost_f.at[6 + i], returned.at[4 + i]) for i in range(2)]
    summed = [back(6 + i, 2 * i - 1, 0, passed.at[i], returned.at[4 + i]) for i in range(2)]
    returns = [
        back(3, -1, outer, ghost_f.at[3], returned.at[1]),
        back(4, 1, outer, ghost_f.at[4], returned.at[2]),
        back(5, 0, outer, ghost_f.at[5], returned.at[3]),
        back(2, 0, inner, ghost_f.at[2], returned.at[0]),
    ]
    second_core = inner < 0

    @pl.when(second_core)
    def _():
        for copy in vias + returns + straight:
            copy.start()

    @pl.when(jnp.logical_not(second_core))
    def _():
        for copy in across + returns:
            copy.start()
        for i, copy in enumerate(vias):
            copy.wait_recv()
            passed[i] = ghost_f[6 + i] + via[i]
            summed[i].start()

    mine = dot(pick_v[8 * g_total :, :], results)
    for c in range(3):
        acc[c] = mine[:, c * 128 : (c + 1) * 128] + self_f[pl.ds(c, leaves, stride=4), :]
    for copy in ahead + out_copies + vias:
        copy.wait_send()
    for copy in returns:
        copy.wait_recv()
    for c in range(3):
        back_f[c] = (returned[0, c] + returned[1, c]) + (returned[2, c] + returned[3, c])
    for copy in straight:
        copy.wait_recv()
    for c in range(3):
        back_f[c] = back_f[c] + (returned[4, c] + returned[5, c])

    @pl.when(second_core)
    def _():
        for copy in across:
            copy.wait_recv()
        for c in range(3):
            back_f[c] = back_f[c] + (returned[6, c] + returned[7, c])

    for c in range(3):
        out_ref[c, 0] = acc[c] + dot(pick_s[...], two(back_f[c]))
    for copy in returns + straight:
        copy.wait_send()


def local(shape, positions, masses, occupancy, export_slots, export_count, pair_list, pair_count):
    leaves, width = masses.shape[1:]
    g_total = export_slots.shape[1]
    pair_slots = pair_list.shape[2]
    far = pl.BlockSpec(memory_space=pltpu.HBM)
    return pl.pallas_call(
        functools.partial(kernel, shape),
        out_shape=pltpu.VMEM(positions.shape, F32),
        in_specs=[far] * 7,
        out_specs=pl.BlockSpec(memory_space=pltpu.VMEM),
        scratch_shapes=[
            pltpu.VMEM((3, leaves, width), F32),
            pltpu.VMEM((leaves, width), F32),
            pltpu.SMEM((1, leaves), jnp.int32),
            pltpu.SMEM((1, g_total), jnp.int32),
            pltpu.SMEM((1, 1), jnp.int32),
            pltpu.SMEM((2, 1, pair_slots), jnp.int32),
            pltpu.SMEM((1, 1), jnp.int32),
            pltpu.VMEM((1, g_total), jnp.int32),
            pltpu.VMEM((2, 1, pair_slots), jnp.int32),
            pltpu.VMEM((g_total, 4, width), F32),
            pltpu.VMEM((leaves + 8 * g_total, 4, width), F32),
            pltpu.VMEM((leaves, 32, width), BF16),
            pltpu.VMEM((leaves, 16, width), BF16),
            pltpu.VMEM((UNROLL, width, width), F32),
            pltpu.VMEM((UNROLL, width, width), F32),
            pltpu.VMEM((2, UNROLL, width, width), BF16),
            pltpu.VMEM((2, UNROLL, width, width), BF16),
            pltpu.VMEM((4 * leaves, width), F32),
            pltpu.VMEM((8 * pair_slots, width), F32),
            pltpu.VMEM((8, 3, g_total, width), F32),
            pltpu.VMEM((2, 3, g_total, width), F32),
            pltpu.VMEM((2, 3, g_total, width), F32),
            pltpu.VMEM((8, 3, g_total, width), F32),
            pltpu.VMEM((3, leaves, width), F32),
            pltpu.VMEM((3, g_total, width), F32),
            pltpu.VMEM((8 * g_total + leaves, 4 * pair_slots), BF16),
            pltpu.VMEM((leaves, 2 * g_total), BF16),
            pltpu.SemaphoreType.DMA((9,)),
            pltpu.SemaphoreType.DMA((8,)),
            pltpu.SemaphoreType.DMA((8,)),
            pltpu.SemaphoreType.DMA((8,)),
            pltpu.SemaphoreType.DMA((8,)),
        ],
        compiler_params=pltpu.CompilerParams(collective_id=0, has_side_effects=True),
    )(positions, masses, occupancy, export_slots, export_count, pair_list, pair_count)


def solution(mesh):
    return jax.shard_map(
        functools.partial(local, (mesh.shape["space"], mesh.shape["sub"])),
        mesh=mesh,
        in_specs=(
            P(None, "space", "sub", None),
            P("space", "sub", None),
            P("space", "sub"),
            P("space", "sub"),
            P("space", "sub"),
            P(None, "space", "sub"),
            P("space", "sub"),
        ),
        out_specs=P(None, "space", "sub", None),
        check_vma=False,
    )
```
